256 devices in a mesh: gx: 8 (over x, core), gy: 8 (over z_lo, y), gz: 4 (over z_hi).
Axes of the slice: x: 4, y: 4, z: 8 (z_hi: 4, z_lo: 2; z = z_hi * 2 + z_lo), core: 2. Of those that a mesh axis runs over, the one named last changes fastest.
Arguments:
- grid_inputs: bfloat16 [186, 512, 1024], P(None, 'gx', 'gy'), may hold values from -6 to 6
- embed_w1: bfloat16 [512, 186], replicated, may hold values from -0.4375 to 0.4375
- embed_b1: float32 [512], replicated, may hold values from -3 to 3
- embed_w2: bfloat16 [512, 512], replicated, may hold values from -0.25 to 0.25
- embed_gain: float32 [512], replicated, may hold values from 0.1 to 1.9
- edge_w1: bfloat16 [512, 1536], replicated, may hold values from -0.15625 to 0.15625
- edge_b1: float32 [512], replicated, may hold values from -3 to 3
- edge_w2: bfloat16 [512, 512], replicated, may hold values from -0.25 to 0.25
- message_gain: float32 [512], replicated, may hold values from 0.1 to 1.9
- message_bias: float32 [512], replicated, may hold values from -3 to 3
- mesh_latent: bfloat16 [512, 8, 8, 256], P('gz', 'gx', 'gy'), may hold values from -6 to 6
- edge_latent: bfloat16 [512, 8, 8, 2048], P('gz', 'gx', 'gy'), may hold values from -6 to 6
- senders: int32 [8, 8, 2048], P('gx', 'gy'), may hold values from 0 to 524287, as said below
- receivers: int32 [8, 8, 2048], P('gx', 'gy'), may hold values from 0 to 16383, as said below
- edge_counts: int32 [8, 8], P('gx', 'gy'), may hold values from 1 to 2048, as said below
Outputs:
- mesh_out: bfloat16 [512, 8, 8, 256], P('gz', 'gx', 'gy')
- grid_latent: bfloat16 [512, 512, 1024], P('gz', 'gx', 'gy')
The draws below stay inside these ranges and needn't reach their ends.
Inputs may be any that keep to these rules, and one draw needn't show every extreme that they name: `senders`: an edge of tile (b, c) has its sender's row within 8 rows of rows b * 64 to (b + 1) * 64 - 1, clipped to the grid, and its column within 8 columns, cyclically, of columns c * 128 to (c + 1) * 128 - 1; this holds in every slot. `receivers`: an edge of tile t is received by a node of that tile, t * 256 to (t + 1) * 256 - 1, in every slot. `edge_counts`: the live edges of a tile are its first slots; some tile holds 2048 live edges.
All inputs are finite; a program needn't handle non-finite values.
Results may differ from the reference program's by a relative error of at most 0.0049.
Values may be sent and summed in bfloat16 or wider, within the bound.
No kernel may reach another device: no remote copies, remote signals or barrier semaphores. Data moves between devices by JAX's collectives and lax.ppermute only.
A program may use at most 128 MiB of HBM per device.

```python
import jax
import jax.numpy as jnp
from jax import lax

LATENT = 512
CHANNELS = 186
GLAT = 64
GLON = 128
MESH_DEV = 256
EDGE_DEV = 2048
HALO = 8
BANDS = 8
SECTORS = 8
NLAT = 512
NLON = 1024


def tile_coords():
    band_ids = jnp.arange(BANDS, dtype=jnp.int32)[:, None, None]
    sector_ids = jnp.arange(SECTORS, dtype=jnp.int32)[None, :, None]
    return (band_ids, sector_ids)


def draw_senders(key, part):
    band_ids, sector_ids = tile_coords()
    lat_key, lon_key = jax.random.split(jax.random.fold_in(key, 11))
    shape = (BANDS, SECTORS, EDGE_DEV)
    rows = jax.random.randint(lat_key, shape, 0, GLAT + 2 * HALO, dtype=jnp.int32) + band_ids * GLAT - HALO
    rows = jnp.clip(rows, 0, NLAT - 1)
    columns = jax.random.randint(lon_key, shape, 0, GLON + 2 * HALO, dtype=jnp.int32) + sector_ids * GLON - HALO + NLON
    columns = columns % NLON
    return (rows * NLON + columns).astype(jnp.int32)


def draw_receivers(key, part):
    band_ids, sector_ids = tile_coords()
    first_key, second_key = jax.random.split(jax.random.fold_in(key, 23))
    shape = (BANDS, SECTORS, EDGE_DEV)
    first = jax.random.randint(first_key, shape, 0, MESH_DEV, dtype=jnp.int32)
    second = jax.random.randint(second_key, shape, 0, MESH_DEV, dtype=jnp.int32)
    return ((band_ids * SECTORS + sector_ids) * MESH_DEV + jnp.minimum(first, second)).astype(jnp.int32)


def draw_edge_counts(key, part):
    band_ids = jnp.arange(BANDS, dtype=jnp.int32)[:, None]
    sector_ids = jnp.arange(SECTORS, dtype=jnp.int32)[None, :]
    distance = jnp.abs(2 * band_ids + 1 - BANDS)
    base = EDGE_DEV // 8 + (EDGE_DEV - EDGE_DEV // 8) * (distance - 1) * (distance - 1) // ((BANDS - 2) * (BANDS - 2))
    jitter_key, pick_key = jax.random.split(jax.random.fold_in(key, 37))
    jitter = jax.random.randint(jitter_key, (BANDS, SECTORS), 0, EDGE_DEV // 64 + 1, dtype=jnp.int32)
    chosen = jax.random.randint(pick_key, (BANDS, 1), 0, SECTORS, dtype=jnp.int32)
    jitter = jnp.where((distance == BANDS - 1) & (sector_ids == chosen), 0, jitter)
    return (base - jitter).astype(jnp.int32)


def steps_of(rng, dims, shards, smallest, top_value):
    loudness = 1.0
    for dim, blocks in shards:
        steps = jax.random.uniform(jax.random.fold_in(jax.random.fold_in(rng, 6), dim), (blocks,), jnp.float32, smallest / len(shards), top_value / len(shards))
        loudness = loudness * jnp.repeat(jnp.exp(steps), dims[dim] // blocks).reshape((-1,) + (1,) * (len(dims) - 1 - dim))
    return loudness


def normal_values(stream_key, dims, width, reach, cuts=(), kind=jnp.bfloat16):
    values = width * jax.random.normal(stream_key, dims, jnp.float32)
    if cuts:
        values = values * steps_of(stream_key, dims, cuts, -0.22, 0.18)
    return jnp.clip(values, -reach, reach).astype(kind)


def setup_inputs(seed: int = 0) -> dict:
    keys = jax.random.split(jax.random.key(seed), 16)
    return {
        "grid_inputs": normal_values(keys[0], (CHANNELS, NLAT, NLON), 1.0, 6.0, ((1, 8), (2, 8))),
        "embed_w1": normal_values(keys[1], (LATENT, CHANNELS), CHANNELS ** -0.5, 0.4375),
        "embed_b1": normal_values(keys[2], (LATENT,), 0.5, 3.0, (), jnp.float32),
        "embed_w2": normal_values(keys[3], (LATENT, LATENT), LATENT ** -0.5, 0.25),
        "embed_gain": jnp.clip(1.0 + 0.18 * jax.random.normal(keys[4], (LATENT,), jnp.float32), 0.1, 1.9),
        "edge_w1": normal_values(keys[5], (LATENT, 3 * LATENT), (3 * LATENT) ** -0.5, 0.15625),
        "edge_b1": normal_values(keys[6], (LATENT,), 0.5, 3.0, (), jnp.float32),
        "edge_w2": normal_values(keys[7], (LATENT, LATENT), LATENT ** -0.5, 0.25),
        "message_gain": jnp.clip(1.0 + 0.18 * jax.random.normal(keys[8], (LATENT,), jnp.float32), 0.1, 1.9),
        "message_bias": normal_values(keys[9], (LATENT,), 0.5, 3.0, (), jnp.float32),
        "mesh_latent": normal_values(keys[10], (LATENT, BANDS, SECTORS, MESH_DEV), 1.0, 6.0, ((0, 4), (1, 8), (2, 8))),
        "edge_latent": normal_values(keys[11], (LATENT, BANDS, SECTORS, EDGE_DEV), 1.0, 6.0, ((0, 4), (1, 8), (2, 8))),
        "senders": draw_senders(jax.random.fold_in(keys[15], 71), 0),
        "receivers": draw_receivers(jax.random.fold_in(keys[15], 71), 0),
        "edge_counts": draw_edge_counts(jax.random.fold_in(keys[15], 71), 0),
    }


epsilon = 1e-05

def normalize(values):
    average = lax.optimization_barrier(jnp.mean(values, axis=0, keepdims=True))
    centred = values - average
    spread = lax.optimization_barrier(jnp.mean(centred * centred, axis=0, keepdims=True))
    return centred * lax.rsqrt(spread + epsilon)

def reference(grid_inputs, embed_w1, embed_b1, embed_w2, embed_gain, edge_w1, edge_b1, edge_w2, message_gain, message_bias, mesh_latent, edge_latent, senders, receivers, edge_counts):
    band_inputs = grid_inputs.reshape(CHANNELS, BANDS, GLAT * NLON).transpose(1, 0, 2)

    def embed_band(block_inputs):
        hidden = jax.nn.silu(jnp.dot(embed_w1, block_inputs, preferred_element_type=jnp.float32) + embed_b1[:, None]).astype(jnp.bfloat16)
        first_pre = jnp.dot(embed_w2, hidden, preferred_element_type=jnp.float32)
        return (normalize(first_pre) * embed_gain[:, None]).astype(jnp.bfloat16)
    band_latent = lax.map(embed_band, band_inputs)
    grid_latent = band_latent.transpose(1, 0, 2).reshape(LATENT, NLAT * NLON)
    tile_count = BANDS * SECTORS
    node_total = tile_count * MESH_DEV
    mesh_flat = mesh_latent.reshape(LATENT, node_total)
    edge_tiles = edge_latent.reshape(LATENT, tile_count, EDGE_DEV).transpose(1, 0, 2)
    send_tiles = senders.reshape(tile_count, EDGE_DEV)
    recv_tiles = receivers.reshape(tile_count, EDGE_DEV)
    count_tiles = edge_counts.reshape(tile_count)
    slot_ids = jnp.arange(EDGE_DEV, dtype=jnp.int32)

    def tile_step(running, inputs):
        totals, degree = running
        edge_cols, send_ids, recv_ids, live_count = inputs
        live_mask = slot_ids < live_count
        stacked = jnp.concatenate([edge_cols, jnp.take(grid_latent, send_ids, axis=1), jnp.take(mesh_flat, recv_ids, axis=1)], axis=0)
        hidden = jax.nn.silu(jnp.dot(edge_w1, stacked, preferred_element_type=jnp.float32) + edge_b1[:, None]).astype(jnp.bfloat16)
        second = jnp.dot(edge_w2, hidden, preferred_element_type=jnp.float32)
        message = (edge_cols.astype(jnp.float32) + normalize(second) * message_gain[:, None] + message_bias[:, None]).astype(jnp.bfloat16)
        weights = jnp.where(live_mask[None, :], message.astype(jnp.float32), jnp.float32(0.0))
        totals = totals + jax.ops.segment_sum(weights.T, recv_ids, num_segments=node_total)
        degree = degree + jax.ops.segment_sum(live_mask.astype(jnp.int32), recv_ids, num_segments=node_total)
        return ((totals, degree), None)
    start_state = (jnp.zeros((node_total, LATENT), jnp.float32), jnp.zeros((node_total,), jnp.int32))
    (totals, degree), unused = lax.scan(tile_step, start_state, (edge_tiles, send_tiles, recv_tiles, count_tiles))
    scale = jnp.maximum(degree, 1).astype(jnp.float32)
    result = mesh_flat.astype(jnp.float32) + totals.T / scale[None, :]
    mesh_out = result.astype(jnp.bfloat16).reshape(LATENT, BANDS, SECTORS, MESH_DEV)
    return (mesh_out, grid_latent.reshape(LATENT, NLAT, NLON))
```

```python
import functools

import jax
import jax.numpy as jnp
from jax import lax
from jax.experimental import pallas as pl
from jax.experimental.pallas import tpu as pltpu
from jax.sharding import PartitionSpec as P

HALO = 8
LANES = 128
DEPTH = 192
ONES = 3

epsilon = 1e-05


def normalized(values):
    scale = 1.0 / values.shape[0]
    average = jnp.sum(values, axis=0, keepdims=True) * scale
    centred = values - average
    spread = jnp.sum(centred * centred, axis=0, keepdims=True) * scale
    return average, lax.rsqrt(spread + epsilon)


def silu_of_half(half):
    return (half + half * jnp.tanh(half)).astype(jnp.bfloat16)


def dot(a, b):
    return jnp.dot(a, b, preferred_element_type=jnp.float32)


def call(body, name, grid=None, **kw):
    return pl.pallas_call(body, name=name, **kw)


def planes_kernel(x_ref, out_ref, left_ref, right_ref, wide_ref, left_acc, right_acc):
    channels, rows, lanes = x_ref.shape
    step = pl.program_id(0)
    wide_ref[...] = x_ref[...].astype(jnp.float32).reshape(channels * rows, lanes)
    extra = DEPTH - channels
    tail_ids = lax.broadcasted_iota(jnp.int32, (extra, lanes), 0)
    tail = jnp.where(tail_ids < ONES, 1.0, 0.0)
    lane_ids = lax.broadcasted_iota(jnp.int32, (DEPTH, lanes), 1)
    group = lanes // HALO
    half = step % (group // rows)
    left = left_acc[...]
    right = right_acc[...]
    for r in range(rows):
        plane = wide_ref[pl.ds(r, channels, stride=rows), :]
        plane = jnp.concatenate([plane, tail], axis=0)
        out_ref[:, r * lanes : (r + 1) * lanes] = plane.astype(jnp.bfloat16)
        first = (half * rows + r) * HALO
        mine = (lane_ids >= first) & (lane_ids < first + HALO)
        left = jnp.where(mine, pltpu.roll(plane, first, 1), left)
        right = jnp.where(mine, pltpu.roll(plane, first + HALO, 1), right)
    left_acc[...] = left
    right_acc[...] = right
    left_ref[...] = left.astype(jnp.bfloat16)
    right_ref[...] = right.astype(jnp.bfloat16)


def planes_of(grid_inputs):
    channels, rows, lanes = grid_inputs.shape
    block = 8
    per_plane = lanes // HALO // block
    packed = jax.ShapeDtypeStruct((DEPTH, rows * HALO), jnp.bfloat16)
    return pl.pallas_call(
        planes_kernel,
        name="planes",
        grid=(rows // block,),
        in_specs=[pl.BlockSpec((channels, block, lanes), lambda i: (0, i, 0))],
        out_specs=[
            pl.BlockSpec((DEPTH, block * lanes), lambda i: (0, i)),
            pl.BlockSpec((DEPTH, lanes), lambda i: (0, i // per_plane)),
            pl.BlockSpec((DEPTH, lanes), lambda i: (0, i // per_plane)),
        ],
        out_shape=[jax.ShapeDtypeStruct((DEPTH, rows * lanes), jnp.bfloat16), packed, packed],
        scratch_shapes=[
            pltpu.VMEM((channels * block, lanes), jnp.float32),
            pltpu.VMEM((DEPTH, lanes), jnp.float32),
            pltpu.VMEM((DEPTH, lanes), jnp.float32),
        ],
    )(grid_inputs)


def corners_kernel(up_ref, down_ref, left_in, right_in, left_ref, right_ref):
    lanes = LANES
    own = left_in.shape[1]
    left_ref[:, :own] = left_in[...]
    right_ref[:, :own] = right_in[...]
    lane_ids = lax.broadcasted_iota(jnp.int32, (DEPTH, lanes), 1)
    left = jnp.zeros((DEPTH, lanes), jnp.float32)
    right = jnp.zeros((DEPTH, lanes), jnp.float32)
    for r in range(2 * HALO):
        source = up_ref if r < HALO else down_ref
        at = (r % HALO) * lanes
        plane = source[:, at : at + lanes].astype(jnp.float32)
        first = r * HALO
        mine = (lane_ids >= first) & (lane_ids < first + HALO)
        left = jnp.where(mine, pltpu.roll(plane, first, 1) if first else plane, left)
        right = jnp.where(mine, pltpu.roll(plane, (first + HALO) % lanes, 1) if (first + HALO) % lanes else plane, right)
    left_ref[:, own:] = left.astype(jnp.bfloat16)
    right_ref[:, own:] = right.astype(jnp.bfloat16)


def with_corners(up, down, left, right):
    packed = jax.ShapeDtypeStruct((DEPTH, left.shape[1] + LANES), jnp.bfloat16)
    return pl.pallas_call(corners_kernel, name="corners", out_shape=[packed, packed])(up, down, left, right)


def embed_kernel(layer_ref, x_ref, w1_ref, wa, wb, wc, wd, gain_ref, *rest, chunk):
    out_ref, acc_ref, wide_ref = rest[-3:]
    keep, rows, lanes = out_ref.shape
    w1 = w1_ref[...]
    gain = gain_ref[...]
    for at in range(0, rows * lanes, chunk):
        hidden = silu_of_half(dot(w1, x_ref[:, at : at + chunk]))
        w2 = jnp.concatenate([wa[...], wb[...], wc[...], wd[...]], axis=0)
        values = dot(w2, hidden)
        average, factor = normalized(values)
        latent = (values[:keep] - average) * factor * gain
        for r in range(chunk // lanes):
            wide_ref[pl.ds(at // lanes + r, keep, stride=rows), :] = latent[:, r * lanes : (r + 1) * lanes]
    out_ref[...] = wide_ref[...].reshape(keep, rows, lanes).astype(jnp.bfloat16)


def embed_rows(layer, planes, w1, w2, gain, rows_total, first, count, earlier=None, block=8, chunk=512):
    latent = w2.shape[0]
    keep = latent // 4
    lanes = LANES
    begin = first // block
    turn = lambda k: (lambda i, s: ((s[0] + k) % 4, 0))
    args = [layer, planes, w1, w2, w2, w2, w2, gain]
    in_specs = [
        pl.BlockSpec((DEPTH, block * lanes), lambda i, s: (0, i + begin)),
        pl.BlockSpec(w1.shape, lambda i, s: (0, 0)),
        pl.BlockSpec((keep, latent), turn(0)),
        pl.BlockSpec((keep, latent), turn(1)),
        pl.BlockSpec((keep, latent), turn(2)),
        pl.BlockSpec((keep, latent), turn(3)),
        pl.BlockSpec((keep, 1), turn(0)),
    ]
    aliases = {}
    if earlier is not None:
        args.append(earlier)
        in_specs.append(pl.BlockSpec(memory_space=pl.ANY))
        aliases = {8: 0}
    cells = count * lanes
    return pl.pallas_call(
        functools.partial(embed_kernel, chunk=chunk),
        name="embed",
        grid_spec=pltpu.PrefetchScalarGridSpec(
            num_scalar_prefetch=1,
            grid=(count // block,),
            in_specs=in_specs,
            out_specs=pl.BlockSpec((keep, block, lanes), lambda i, s: (0, i + begin, 0)),
            scratch_shapes=[
                pltpu.VMEM((8, 128), jnp.float32),
                pltpu.VMEM((keep * block, lanes), jnp.float32),
            ],
        ),
        out_shape=jax.ShapeDtypeStruct((keep, rows_total, lanes), jnp.bfloat16),
        input_output_aliases=aliases,
        cost_estimate=pl.CostEstimate(
            flops=2 * cells * latent * (256 + latent), transcendentals=cells * latent, bytes_accessed=cells * 640
        ),
    )(*args)


def sender_kernel(pick_ref, x_ref, up_ref, down_ref, left_ref, right_ref, w1_ref, w2_ref, gain_ref, out_ref):
    slots = pick_ref.shape[1]
    pick = pick_ref[...]

    def picked(ref, begin, at, width):
        ids = lax.broadcasted_iota(jnp.int32, (width, slots), 0) + (begin + at)
        chosen = jnp.where(ids == pick, 1.0, 0.0).astype(jnp.bfloat16)
        return dot(ref[:, at : at + width], chosen)

    total = jnp.zeros((DEPTH, slots), jnp.float32)
    begin = 0
    for ref in (x_ref, up_ref, down_ref, left_ref, right_ref):
        size = ref.shape[1]
        width = min(size, 1024)
        for at in range(0, size, width):
            total = total + picked(ref, begin, at, width)
        begin += size
    hidden = silu_of_half(dot(w1_ref[...], total.astype(jnp.bfloat16)))
    values = dot(w2_ref[...], hidden)
    average, factor = normalized(values)
    out_ref[...] = ((values - average) * factor * gain_ref[...]).astype(jnp.bfloat16)


def sender_latents(pick, planes, up, down, left, right, w1, w2, gain):
    slots = pick.shape[1]
    latent = w2.shape[0]
    cells = planes.shape[1] + 2 * up.shape[1] + 2 * left.shape[1]
    return pl.pallas_call(
        sender_kernel,
        name="senders",
        out_shape=jax.ShapeDtypeStruct((latent, slots), jnp.bfloat16),
        cost_estimate=pl.CostEstimate(flops=2 * cells * 256 * slots, transcendentals=0, bytes_accessed=cells * 400),
    )(pick, planes, up, down, left, right, w1, w2, gain)


def edge_kernel(live_ref, near_ref, all_near_ref, in_ref, send_ref, w1_ref, b1_ref, w2_ref, gain_ref, bias_ref, out_ref, degree_ref):
    latent = w2_ref.shape[0]
    slots = near_ref.shape[1]
    nodes = out_ref.shape[1]
    edge = in_ref[:, :slots]
    mesh = in_ref[:, slots:]
    near = near_ref[...]
    node_ids = lax.broadcasted_iota(jnp.int32, (nodes, slots), 0)
    onehot = jnp.where(node_ids == near, 1.0, 0.0).astype(jnp.bfloat16)
    mesh_cols = dot(mesh, onehot).astype(jnp.bfloat16)
    first = dot(w1_ref[:, :latent], edge) + dot(w1_ref[:, latent : 2 * latent], send_ref[...])
    first = first + dot(w1_ref[:, 2 * latent :], mesh_cols) + b1_ref[...]
    hidden = silu_of_half(0.5 * first)
    second = dot(w2_ref[...], hidden)
    average, factor = normalized(second)
    message = edge.astype(jnp.float32) + (second - average) * factor * gain_ref[...] + bias_ref[...]
    slot_ids = lax.broadcasted_iota(jnp.int32, (nodes, slots), 1) + live_ref[1]
    counted = jnp.where((node_ids == near) & (slot_ids < live_ref[0]), 1.0, 0.0).astype(jnp.bfloat16)
    nt = (((1,), (1,)), ((), ()))
    out_ref[...] = lax.dot_general(
        message.astype(jnp.bfloat16), counted, nt, preferred_element_type=jnp.float32
    ).astype(jnp.bfloat16)
    every = all_near_ref.shape[1]
    node_all = lax.broadcasted_iota(jnp.int32, (nodes, every), 0)
    slot_all = lax.broadcasted_iota(jnp.int32, (nodes, every), 1)
    counted_all = jnp.where((node_all == all_near_ref[...]) & (slot_all < live_ref[0]), 1.0, 0.0).astype(jnp.bfloat16)
    degree_ref[...] = lax.dot_general(
        jnp.ones((8, every), jnp.bfloat16), counted_all, nt, preferred_element_type=jnp.float32
    )


def edge_sums(live, near, all_near, arrived, send, w1, b1, w2, gain, bias, nodes):
    latent = w2.shape[0]
    vmem = pl.BlockSpec(memory_space=pltpu.VMEM)
    return pl.pallas_call(
        edge_kernel,
        name="edges",
        in_specs=[pl.BlockSpec(memory_space=pltpu.SMEM)] + [vmem] * 9,
        out_shape=[
            jax.ShapeDtypeStruct((latent, nodes), jnp.bfloat16),
            jax.ShapeDtypeStruct((8, nodes), jnp.float32),
        ],
        cost_estimate=pl.CostEstimate(
            flops=2 * near.shape[1] * latent * (5 * latent), transcendentals=0, bytes_accessed=1 << 22
        ),
    )(live, near, all_near, arrived, send, w1, b1, w2, gain, bias)


def with_bias_columns(weight, bias):
    parts = []
    left = bias
    for _ in range(ONES):
        part = lax.reduce_precision(left, 8, 7)
        parts.append(part)
        left = left - part
    rest = DEPTH - weight.shape[1] - ONES
    columns = jnp.stack(parts + [jnp.zeros_like(bias)] * rest, axis=1)
    return jnp.concatenate([weight, columns.astype(jnp.bfloat16)], axis=1) * jnp.bfloat16(0.5)


def shifted(value, axis, by):
    size = lax.axis_size(axis)
    return lax.ppermute(value, axis, [(i, (i + by) % size) for i in range(size)])


def on_device(
    grid_inputs,
    embed_w1,
    embed_b1,
    embed_w2,
    embed_gain,
    edge_w1,
    edge_b1,
    edge_w2,
    message_gain,
    message_bias,
    mesh_latent,
    edge_latent,
    senders,
    receivers,
    edge_counts,
):
    latent = embed_w2.shape[0]
    shard_rows = mesh_latent.shape[0]
    lat_rows, lon_cols = grid_inputs.shape[1:]
    node_count = mesh_latent.shape[3]
    slot_count = edge_latent.shape[3]
    layers = lax.axis_size("gz")
    share = slot_count // layers
    layer = lax.axis_index("gz")
    band = lax.axis_index("gx")
    sector = lax.axis_index("gy")
    lon_total = lon_cols * lax.axis_size("gy")
    live_count = edge_counts[0, 0]
    mesh_own = mesh_latent[:, 0, 0, :]
    edge_own = edge_latent[:, 0, 0, :]

    shares = edge_own.reshape(shard_rows, layers, share).transpose(1, 0, 2)
    outgoing = jnp.concatenate(
        [shares, jnp.broadcast_to(mesh_own[None], (layers, shard_rows, node_count))], axis=2
    )
    arrived = lax.all_to_all(outgoing, "gz", 0, 0, tiled=True).reshape(latent, share + node_count)

    planes, left, right = planes_of(grid_inputs)
    width = HALO * lon_cols
    from_up = shifted(planes[:, -width:], "gx", 1)
    from_down = shifted(planes[:, :width], "gx", -1)
    left, right = with_corners(from_up, from_down, left, right)
    from_left = shifted(right, "gy", 1)
    from_right = shifted(left, "gy", -1)

    mine = lambda a: lax.dynamic_slice_in_dim(a, layer * share, share, 0)[None]
    send_all = mine(senders[0, 0])
    lat = send_all // lon_total - band * lat_rows
    lon = (send_all % lon_total - sector * lon_cols + HALO + lon_total) % lon_total - HALO
    inside_lon = (lon >= 0) & (lon < lon_cols)
    own = lat_rows * lon_cols
    side = (lat_rows + 2 * HALO) * HALO
    at_row = jnp.where(
        lat < 0, own + (lat + HALO) * lon_cols, jnp.where(lat < lat_rows, lat * lon_cols, own + width + (lat - lat_rows) * lon_cols)
    )
    at_side = jnp.where(
        lat < 0, (lat_rows + lat + HALO) * HALO, jnp.where(lat < lat_rows, lat * HALO, (lat + HALO) * HALO)
    )
    at_side = at_side + own + 2 * width
    pick = jnp.where(
        inside_lon, at_row + lon, jnp.where(lon < 0, at_side + lon + HALO, at_side + side + lon - lon_cols)
    )
    tile = band * lax.axis_size("gy") + sector
    near_all = receivers[0] - tile * node_count
    near = mine(near_all[0])

    w1 = with_bias_columns(embed_w1, embed_b1)
    gain = embed_gain[:, None]
    layer_arg = layer.astype(jnp.int32)[None]
    embed = functools.partial(embed_rows, layer_arg, planes, w1, embed_w2, gain, lat_rows)
    grid_out = embed(0, 24)
    grid_out = embed(24, 24, grid_out)
    send = sender_latents(pick, planes, from_up, from_down, from_left, from_right, w1, embed_w2, gain)
    live = jnp.stack([live_count, (layer * share).astype(jnp.int32)])
    sums, degree = edge_sums(
        live, near, near_all, arrived, send, edge_w1, edge_b1[:, None], edge_w2,
        message_gain[:, None], message_bias[:, None], node_count,
    )
    parts = lax.all_to_all(sums.reshape(layers, shard_rows, node_count), "gz", 0, 0, tiled=True)
    grid_out = embed(48, 16, grid_out)
    totals = parts.astype(jnp.float32).sum(axis=0)
    result = mesh_own.astype(jnp.float32) + totals / jnp.maximum(degree[:1], 1.0)
    return (result.astype(jnp.bfloat16).reshape(shard_rows, 1, 1, node_count), grid_out)


def solution(mesh):
    return jax.shard_map(
        on_device,
        mesh=mesh,
        in_specs=(
            P(None, "gx", "gy"),
            P(),
            P(),
            P(),
            P(),
            P(),
            P(),
            P(),
            P(),
            P(),
            P("gz", "gx", "gy", None),
            P("gz", "gx", "gy", None),
            P("gx", "gy", None),
            P("gx", "gy", None),
            P("gx", "gy"),
        ),
        out_specs=(P("gz", "gx", "gy", None), P("gz", "gx", "gy")),
        check_vma=False,
    )
```

```python
import functools

import jax
import jax.numpy as jnp
from jax import lax
from jax.experimental import pallas as pl
from jax.experimental.pallas import tpu as pltpu
from jax.sharding import PartitionSpec as P


HALO = 8
LANES = 128
DEPTH = 192
ONES = 3
CHUNK = 16

epsilon = 1e-05


def normalized(values):
    scale = 1.0 / values.shape[0]
    average = jnp.sum(values, axis=0, keepdims=True) * scale
    centred = values - average
    spread = jnp.sum(centred * centred, axis=0, keepdims=True) * scale
    return average, lax.rsqrt(spread + epsilon)


def silu_of_half(half):
    return (half + half * jnp.tanh(half)).astype(jnp.bfloat16)


def dot(a, b):
    return jnp.dot(a, b, preferred_element_type=jnp.float32)


VMEM = pl.BlockSpec(memory_space=pltpu.VMEM)
HBM = pl.BlockSpec(memory_space=pltpu.HBM)


def on_chip(value):
    return pltpu.with_memory_space_constraint(value, pltpu.VMEM)


def off_chip(value):
    return pltpu.with_memory_space_constraint(value, pltpu.HBM)


WIDE = HALO * LANES
VECTORS = 4
EARLY = 40


def column(late_ref, begin, count, latent, which):
    at = latent + 2 * LANES
    parts = [
        late_ref[pl.ds(begin, count), at + n * VECTORS + which : at + n * VECTORS + which + 1].astype(jnp.float32)
        for n in range(ONES)
    ]
    return parts[0] + parts[1] + parts[2]


def plane_group(early_ref, late_ref, g):
    k = g - EARLY // HALO
    return early_ref[g * DEPTH : (g + 1) * DEPTH, :] if k < 0 else late_ref[k * DEPTH : (k + 1) * DEPTH, :]


def three_parts(value):
    parts = []
    for _ in range(ONES):
        part = value.astype(jnp.bfloat16).astype(jnp.float32)
        parts.append(part)
        value = value - part
    return parts


def prepare_kernel(x_ref, w1_ref, b1_ref, gain_ref, edge_b1_ref, message_gain_ref, message_bias_ref, w2_ref,
                   edge_ref, mesh_ref, early_ref, late_ref, top_ref, low_ref, *rest):
    going_refs = rest[:-11]
    (x_in, w1_in, vectors_in, edge_in, mesh_in, in_sem, early_sem, weight_sem, edge_sem, going_sem, out_sem) = rest[-11:]
    channels, rows, lanes = x_ref.shape
    latent = w2_ref.shape[0]
    group = CHUNK
    steps = DEPTH // group
    low = (rows - EARLY) // HALO * DEPTH
    end = low + latent
    sources = [w1_ref, b1_ref, gain_ref, edge_b1_ref, message_gain_ref, message_bias_ref]
    targets = [w1_in] + [vectors_in.at[n] for n in range(5)]
    early = [pltpu.make_async_copy(s, t, early_sem.at[n]) for n, (s, t) in enumerate(zip(sources, targets))]
    for copy in early:
        copy.start()
    incoming = []
    for k in range(steps):
        size = min(group, channels - k * group)
        copy = pltpu.make_async_copy(
            x_ref.at[pl.ds(k * group, size)], x_in.at[pl.ds(k * group, size)], in_sem.at[k]
        )
        copy.start()
        incoming.append(copy)
    layers = len(going_refs) + 1
    _, joined = going_refs[0].shape
    share = edge_in.shape[1] // layers
    layer = lax.axis_index("gz")
    features = [
        pltpu.make_async_copy(edge_ref, edge_in, edge_sem.at[0]),
        pltpu.make_async_copy(mesh_ref, mesh_in, edge_sem.at[1]),
    ]
    for copy in features:
        copy.start()
    weight = pltpu.make_async_copy(w2_ref, late_ref.at[pl.ds(low, latent), pl.ds(0, latent)], weight_sem)
    weight.start()
    for copy in early:
        copy.wait()
    stacked = []
    split = [three_parts(vectors_in[n]) for n in range(1, 1 + VECTORS)]
    for n in range(ONES):
        stacked += [parts[n] for parts in split]
    stacked.append(jnp.zeros((lanes - len(stacked), latent), jnp.float32))
    at = latent + 2 * lanes
    late_ref[low:end, at : at + lanes] = jnp.transpose(jnp.concatenate(stacked, axis=0)).astype(jnp.bfloat16)
    bias = three_parts(vectors_in[0]) + [jnp.zeros((DEPTH - channels - ONES, latent), jnp.float32)]
    full = jnp.concatenate([w1_in[...].astype(jnp.float32)] + bias, axis=0) * 0.5
    late_ref[low:end, latent : latent + DEPTH] = jnp.transpose(full).astype(jnp.bfloat16)

    for copy in features:
        copy.wait()
    going = []
    for j, target in enumerate(going_refs):
        first = pl.multiple_of((layer + j + 1) % layers * share, share)
        pair = [
            (edge_in.at[:, pl.ds(first, share)], target.at[:, pl.ds(0, share)]),
            (mesh_in, target.at[:, pl.ds(share, joined - share)]),
        ]
        going += [pltpu.make_async_copy(s, t, going_sem.at[2 * j + n]) for n, (s, t) in enumerate(pair)]
    for copy in going:
        copy.start()

    row_ids = lax.broadcasted_iota(jnp.int32, (group, lanes), 0)
    for k in range(steps):
        incoming[k].wait()
        cells = jnp.swapaxes(x_in[k * group : (k + 1) * group], 0, 1)
        for r in range(rows):
            plane = cells[r]
            if (k + 1) * group > channels:
                ids = row_ids + k * group
                wide = plane.astype(jnp.float32)
                wide = jnp.where(ids < channels, wide, jnp.where(ids < channels + ONES, 1.0, 0.0))
                plane = wide.astype(jnp.bfloat16)
            target, row = (early_ref, r) if r < EARLY else (late_ref, r - EARLY)
            down = row // HALO * DEPTH + k * group
            over = r % HALO * lanes
            target[down : down + group, over : over + lanes] = plane
    ends = [
        pltpu.make_async_copy(early_ref.at[pl.ds(0, DEPTH), :], top_ref, out_sem.at[0]),
        pltpu.make_async_copy(late_ref.at[pl.ds(low - DEPTH, DEPTH), :], low_ref, out_sem.at[1]),
    ]
    for copy in ends:
        copy.start()
    for copy in [weight] + going + ends:
        copy.wait()


def prepare(grid_inputs, w1, b1, gain, edge_b1, message_gain, message_bias, w2, edge_own, mesh_own, layers):
    channels, rows, lanes = grid_inputs.shape
    latent = w1.shape[0]
    steps = DEPTH // CHUNK
    shard, slots = edge_own.shape
    strip = pltpu.HBM((DEPTH, WIDE), jnp.bfloat16)
    vectors = [a[None] for a in (b1, gain, edge_b1, message_gain, message_bias)]
    return pl.pallas_call(
        prepare_kernel,
        name="prepare",
        compiler_params=pltpu.CompilerParams(vmem_limit_bytes=24 << 20),
        in_specs=[HBM] * 10,
        out_specs=[VMEM, VMEM] + [HBM] * (layers + 1),
        out_shape=[
            pltpu.VMEM((EARLY // HALO * DEPTH, WIDE), jnp.bfloat16),
            pltpu.VMEM(((rows - EARLY) // HALO * DEPTH + latent, WIDE), jnp.bfloat16),
            strip,
            strip,
        ] + [pltpu.HBM((shard, slots // layers + mesh_own.shape[1]), jnp.bfloat16)] * (layers - 1),
        scratch_shapes=[
            pltpu.VMEM((DEPTH, rows, lanes), jnp.bfloat16),
            pltpu.VMEM((channels, latent), jnp.bfloat16),
            pltpu.VMEM((5, 1, latent), jnp.float32),
            pltpu.VMEM(edge_own.shape, jnp.bfloat16),
            pltpu.VMEM(mesh_own.shape, jnp.bfloat16),
            pltpu.SemaphoreType.DMA((steps,)),
            pltpu.SemaphoreType.DMA((6,)),
            pltpu.SemaphoreType.DMA,
            pltpu.SemaphoreType.DMA((2,)),
            pltpu.SemaphoreType.DMA((2 * layers - 2,)),
            pltpu.SemaphoreType.DMA((2,)),
        ],
    )(*[off_chip(a) for a in [grid_inputs, w1.T] + vectors + [w2, edge_own, mesh_own]])


def corners_kernel(early_ref, late_ref, up_ref, down_ref, left_ref, right_ref, *, rows):
    lanes = LANES
    per = lanes // HALO
    lane_ids = lax.broadcasted_iota(jnp.int32, (DEPTH, lanes), 1)
    for r in range(rows + 2 * HALO):
        over = r % HALO * lanes
        if r < rows:
            plane = plane_group(early_ref, late_ref, r // HALO)[:, over : over + lanes]
        else:
            plane = (up_ref if r < rows + HALO else down_ref)[:, over : over + lanes]
        plane = plane.astype(jnp.float32)
        first = r % per * HALO
        again = (first + HALO) % lanes
        mine = (lane_ids >= first) & (lane_ids < first + HALO)
        moved = pltpu.roll(plane, first, 1) if first else plane
        moved_too = pltpu.roll(plane, again, 1) if again else plane
        left = moved if r % per == 0 else jnp.where(mine, moved, left)
        right = moved_too if r % per == 0 else jnp.where(mine, moved_too, right)
        if r % per == per - 1:
            place = slice(r // per * lanes, (r // per + 1) * lanes)
            left_ref[:, place] = left.astype(jnp.bfloat16)
            right_ref[:, place] = right.astype(jnp.bfloat16)


def corners(early, late, up, down, rows):
    packed = pltpu.VMEM((DEPTH, (rows + 2 * HALO) * HALO), jnp.bfloat16)
    return pl.pallas_call(
        functools.partial(corners_kernel, rows=rows),
        name="corners",
        compiler_params=pltpu.CompilerParams(vmem_limit_bytes=8 << 20),
        in_specs=[VMEM] * 4,
        out_specs=[VMEM] * 2,
        out_shape=[packed, packed],
    )(on_chip(early), on_chip(late), on_chip(up), on_chip(down))


def embed_kernel(x_ref, late_ref, *rest, first, latent):
    out_ref, wide_ref = rest[-2:]
    keep, rows, lanes = out_ref.shape
    layers = latent // keep
    layer = lax.axis_index("gz")
    low = late_ref.shape[0] - latent
    w1 = late_ref[low:, latent : latent + DEPTH]
    begin = lambda k: pl.multiple_of(low + (layer + k) % layers * keep, keep)
    w2 = jnp.concatenate([late_ref[pl.ds(begin(k), keep), :latent] for k in range(layers)], axis=0)
    gain = column(late_ref, begin(0), keep, latent, 0)
    here = pl.multiple_of((pl.program_id(0) + first) * DEPTH, DEPTH)
    hidden = silu_of_half(dot(w1, x_ref[pl.ds(here, DEPTH), :]))
    values = dot(w2, hidden)
    average, factor = normalized(values)
    done = (values[:keep] - average) * factor * gain
    for r in range(rows):
        wide_ref[pl.ds(r, keep, stride=rows), :] = done[:, r * lanes : (r + 1) * lanes]
    out_ref[...] = wide_ref[...].reshape(keep, rows, lanes).astype(jnp.bfloat16)


def embed_rows(early, late, latent, keep, rows_total, first, count, earlier=None):
    begin = first // HALO
    source, start = (early, begin) if first < EARLY else (late, begin - EARLY // HALO)
    args = [on_chip(source), on_chip(late)]
    in_specs = [VMEM] * 2
    aliases = {}
    if earlier is not None:
        args.append(off_chip(earlier))
        in_specs.append(HBM)
        aliases = {2: 0}
    cells = count * LANES
    return pl.pallas_call(
        functools.partial(embed_kernel, first=start, latent=latent),
        name="embed",
        compiler_params=pltpu.CompilerParams(vmem_limit_bytes=24 << 20),
        grid=(count // HALO,),
        in_specs=in_specs,
        out_specs=pl.BlockSpec((keep, HALO, LANES), lambda i: (0, i + begin, 0)),
        scratch_shapes=[pltpu.VMEM((keep * HALO, LANES), jnp.float32)],
        out_shape=jax.ShapeDtypeStruct((keep, rows_total, LANES), jnp.bfloat16),
        input_output_aliases=aliases,
        cost_estimate=pl.CostEstimate(
            flops=2 * cells * latent * (256 + latent), transcendentals=cells * latent, bytes_accessed=cells * 640
        ),
    )(*args)


def edge_kernel(count_ref, senders_ref, receivers_ref, early_ref, late_ref, up_ref, down_ref, left_ref, right_ref, *rest,
                lon_bits, rows, layers):
    piece_refs = rest[: layers - 1]
    edge_ref, mesh_ref, w1_ref, w2_ref = rest[layers - 1 : layers + 3]
    own_ref, *sum_refs, degree_ref = rest[layers + 3 : 2 * layers + 4]
    w1_in, w2_in, arrived, sums, sem = rest[2 * layers + 4 :]
    latent, joined = arrived.shape
    shard, nodes = own_ref.shape
    slots = joined - nodes
    lanes = LANES
    layer = lax.axis_index("gz")
    band = lax.axis_index("gx")
    sector = lax.axis_index("gy")
    start = pl.multiple_of(layer * slots, slots)
    place = lambda j: pl.ds(pl.multiple_of((layer + j) % layers * shard, shard), shard)
    pairs = [
        (edge_ref.at[:, pl.ds(start, slots)], arrived.at[place(0), pl.ds(0, slots)]),
        (mesh_ref, arrived.at[place(0), pl.ds(slots, nodes)]),
        (w1_ref, w1_in),
        (w2_ref, w2_in),
    ]
    copies = [pltpu.make_async_copy(s, t, sem.at[n]) for n, (s, t) in enumerate(pairs)]
    for copy in copies:
        copy.start()
    for j, piece in enumerate(piece_refs):
        arrived[place(layers - 1 - j), :] = piece[...]

    low = late_ref.shape[0] - latent
    vector = lambda n: column(late_ref, low, latent, latent, n)
    cell = senders_ref[:, pl.ds(start, slots)]
    lon_total = 1 << lon_bits
    lat = lax.shift_right_logical(cell, lon_bits) - band * rows
    lon = ((cell & (lon_total - 1)) - sector * lanes + HALO & (lon_total - 1)) - HALO
    own = rows * lanes
    side = (rows + 2 * HALO) * HALO
    at_row = jnp.where(
        lat < 0, own + (lat + HALO) * lanes, jnp.where(lat < rows, lat * lanes, own + WIDE + (lat - rows) * lanes)
    )
    at_side = own + 2 * WIDE + HALO * jnp.where(lat < 0, rows + lat + HALO, jnp.where(lat < rows, lat, lat + HALO))
    pick = jnp.where(
        (lon >= 0) & (lon < lanes), at_row + lon, jnp.where(lon < 0, at_side + lon + HALO, at_side + side + lon - lanes)
    )
    planes = [plane_group(early_ref, late_ref, g) for g in range(rows // HALO)]
    total = jnp.zeros((DEPTH, slots), jnp.float32)
    begin = 0
    for part in planes + [up_ref[...], down_ref[...], left_ref[...], right_ref[...]]:
        size = part.shape[1]
        ids = lax.broadcasted_iota(jnp.int32, (size, slots), 0) + begin
        total = total + dot(part, jnp.where(ids == pick, 1.0, 0.0).astype(jnp.bfloat16))
        begin += size
    hidden = silu_of_half(dot(late_ref[low:, latent : latent + DEPTH], total.astype(jnp.bfloat16)))
    values = dot(late_ref[low:, :latent], hidden)
    average, factor = normalized(values)
    send = ((values - average) * factor * vector(0)).astype(jnp.bfloat16)

    tile = band * lax.axis_size("gy") + sector
    live = count_ref[0, 0]
    nt = (((1,), (1,)), ((), ()))
    every = receivers_ref.shape[1]
    slot_all = lax.broadcasted_iota(jnp.int32, (1, every), 1)
    near_all = jnp.where(slot_all < live, receivers_ref[...] - tile * nodes, -1)
    node_all = lax.broadcasted_iota(jnp.int32, (nodes, every), 0)
    counted_all = jnp.where(node_all == near_all, 1.0, 0.0).astype(jnp.bfloat16)
    degree_ref[...] = lax.dot_general(
        jnp.ones((8, every), jnp.bfloat16), counted_all, nt, preferred_element_type=jnp.float32
    )
    near = receivers_ref[:, pl.ds(start, slots)] - tile * nodes
    node_ids = lax.broadcasted_iota(jnp.int32, (nodes, slots), 0)
    onehot = jnp.where(node_ids == near, 1.0, 0.0).astype(jnp.bfloat16)
    slot_ids = lax.broadcasted_iota(jnp.int32, (1, slots), 1) + start
    counted = jnp.where(node_ids == jnp.where(slot_ids < live, near, -1), 1.0, 0.0).astype(jnp.bfloat16)
    for copy in copies:
        copy.wait()
    edge = arrived[:, :slots]
    mesh_cols = dot(arrived[:, slots:], onehot).astype(jnp.bfloat16)
    stacked = jnp.concatenate([edge, send, mesh_cols], axis=0)
    hidden = silu_of_half(0.5 * (dot(w1_in[...], stacked) + vector(1)))
    second = dot(w2_in[...], hidden)
    average, factor = normalized(second)
    message = edge.astype(jnp.float32) + (second - average) * factor * vector(2) + vector(3)
    sums[...] = lax.dot_general(message.astype(jnp.bfloat16), counted, nt, preferred_element_type=jnp.float32)
    own_ref[...] = sums[place(0), :]
    for j, target in enumerate(sum_refs):
        target[...] = sums[place(j + 1), :].astype(jnp.bfloat16)


def edge_sums(count, senders, receivers, early, late, up, down, left, right, pieces, edge_own, mesh_own, w1, w2,
              rows, lon_total):
    latent = w2.shape[0]
    layers = len(pieces) + 1
    shard, nodes = mesh_own.shape
    slots = edge_own.shape[1] // layers
    near_by = [on_chip(a) for a in (early, late, up, down, left, right, *pieces)]
    far = [off_chip(a) for a in (edge_own, mesh_own, w1, w2)]
    return pl.pallas_call(
        functools.partial(edge_kernel, lon_bits=lon_total.bit_length() - 1, rows=rows, layers=layers),
        name="edges",
        compiler_params=pltpu.CompilerParams(vmem_limit_bytes=32 << 20),
        in_specs=[pl.BlockSpec(memory_space=pltpu.SMEM)] + [VMEM] * (2 + len(near_by)) + [HBM] * 4,
        out_specs=[VMEM] * (layers + 1),
        out_shape=[pltpu.VMEM((shard, nodes), jnp.float32)]
        + [pltpu.VMEM((shard, nodes), jnp.bfloat16)] * (layers - 1)
        + [pltpu.VMEM((8, nodes), jnp.float32)],
        scratch_shapes=[
            pltpu.VMEM(w1.shape, jnp.bfloat16),
            pltpu.VMEM(w2.shape, jnp.bfloat16),
            pltpu.VMEM((latent, slots + nodes), jnp.bfloat16),
            pltpu.VMEM((latent, nodes), jnp.float32),
            pltpu.SemaphoreType.DMA((4,)),
        ],
        cost_estimate=pl.CostEstimate(flops=6 * 10**9, transcendentals=0, bytes_accessed=1 << 22),
    )(count, senders, receivers, *near_by, *far)


def finish_kernel(own_ref, *rest):
    *part_refs, degree_ref, mesh_ref, out_ref = rest
    totals = own_ref[...]
    for part in part_refs:
        totals = totals + part[...].astype(jnp.float32)
    scale = jnp.maximum(degree_ref[0:1, :], 1.0)
    out_ref[...] = (mesh_ref[...].astype(jnp.float32) + totals / scale).astype(jnp.bfloat16)


def finish(own, parts, degree, mesh_own):
    args = [on_chip(a) for a in (own, *parts, degree, mesh_own)]
    return pl.pallas_call(
        finish_kernel,
        name="finish",
        compiler_params=pltpu.CompilerParams(vmem_limit_bytes=8 << 20),
        in_specs=[VMEM] * len(args),
        out_specs=VMEM,
        out_shape=jax.ShapeDtypeStruct(mesh_own.shape, jnp.bfloat16),
    )(*args)


def shifted(value, axis, by):
    size = lax.axis_size(axis)
    return lax.ppermute(value, axis, [(i, (i + by) % size) for i in range(size)])


def on_device(
    grid_inputs,
    embed_w1,
    embed_b1,
    embed_w2,
    embed_gain,
    edge_w1,
    edge_b1,
    edge_w2,
    message_gain,
    message_bias,
    mesh_latent,
    edge_latent,
    senders,
    receivers,
    edge_counts,
):
    latent = embed_w2.shape[0]
    shard_rows = mesh_latent.shape[0]
    lat_rows, lon_cols = grid_inputs.shape[1:]
    node_count = mesh_latent.shape[3]
    layers = lax.axis_size("gz")
    lon_total = lon_cols * lax.axis_size("gy")
    mesh_own = mesh_latent[:, 0, 0, :]
    edge_own = edge_latent[:, 0, 0, :]

    early, late, top, low, *outgoing = prepare(
        grid_inputs, embed_w1, embed_b1, embed_gain, edge_b1, message_gain, message_bias, embed_w2, edge_own, mesh_own,
        layers,
    )
    embed = functools.partial(embed_rows, early, late, latent, shard_rows, lat_rows)
    from_up = shifted(low, "gx", 1)
    from_down = shifted(top, "gx", -1)
    pieces = [shifted(piece, "gz", j + 1) for j, piece in enumerate(outgoing)]
    grid_out = embed(0, 16)
    from_up, from_down, grid_out = lax.optimization_barrier((from_up, from_down, grid_out))
    left, right = corners(early, late, from_up, from_down, lat_rows)
    from_left = shifted(right, "gy", 1)
    from_right = shifted(left, "gy", -1)
    grid_out = embed(16, EARLY - 16, grid_out)
    from_left, from_right, grid_out = lax.optimization_barrier((from_left, from_right, grid_out))
    own, *sums, degree = edge_sums(
        edge_counts, senders[0], receivers[0], early, late, from_up, from_down, from_left, from_right, pieces,
        edge_own, mesh_own, edge_w1, edge_w2, lat_rows, lon_total,
    )
    parts = [shifted(part, "gz", j + 1) for j, part in enumerate(sums)]
    grid_out = embed(EARLY, lat_rows - EARLY, grid_out)
    *parts, grid_out = lax.optimization_barrier((*parts, grid_out))
    result = finish(own, parts, degree, mesh_own)
    return (result.reshape(shard_rows, 1, 1, node_count), grid_out)


def solution(mesh):
    return jax.shard_map(
        on_device,
        mesh=mesh,
        in_specs=(
            P(None, "gx", "gy"),
            P(),
            P(),
            P(),
            P(),
            P(),
            P(),
            P(),
            P(),
            P(),
            P("gz", "gx", "gy", None),
            P("gz", "gx", "gy", None),
            P("gx", "gy", None),
            P("gx", "gy", None),
            P("gx", "gy"),
        ),
        out_specs=(P("gz", "gx", "gy", None), P("gz", "gx", "gy")),
        check_vma=False,
    )
```

```python
import functools

import jax
import jax.numpy as jnp
from jax import lax
from jax.experimental import pallas as pl
from jax.experimental.pallas import tpu as pltpu
from jax.sharding import PartitionSpec as P


HALO = 8
LANES = 128
DEPTH = 192
ONES = 3
CHUNK = 16

epsilon = 1e-05


def normalized(values):
    scale = 1.0 / values.shape[0]
    average = jnp.sum(values, axis=0, keepdims=True) * scale
    centred = values - average
    spread = jnp.sum(centred * centred, axis=0, keepdims=True) * scale
    return average, lax.rsqrt(spread + epsilon)


def silu_of_half(half):
    return (half + half * jnp.tanh(half)).astype(jnp.bfloat16)


def dot(a, b):
    return jnp.dot(a, b, preferred_element_type=jnp.float32)


VMEM = pl.BlockSpec(memory_space=pltpu.VMEM)
HBM = pl.BlockSpec(memory_space=pltpu.HBM)


def on_chip(value):
    return pltpu.with_memory_space_constraint(value, pltpu.VMEM)


def off_chip(value):
    return pltpu.with_memory_space_constraint(value, pltpu.HBM)


WIDE = HALO * LANES
VECTORS = 4
EARLY = 32


def column(late_ref, begin, count, latent, which):
    at = latent + 2 * LANES
    parts = [
        late_ref[pl.ds(begin, count), at + n * VECTORS + which : at + n * VECTORS + which + 1].astype(jnp.float32)
        for n in range(ONES)
    ]
    return parts[0] + parts[1] + parts[2]


def plane_group(early_ref, late_ref, g):
    k = g - EARLY // HALO
    return early_ref[g * DEPTH : (g + 1) * DEPTH, :] if k < 0 else late_ref[k * DEPTH : (k + 1) * DEPTH, :]


def three_parts(value):
    parts = []
    for _ in range(ONES):
        part = value.astype(jnp.bfloat16).astype(jnp.float32)
        parts.append(part)
        value = value - part
    return parts


def prepare_kernel(x_ref, w1_ref, b1_ref, gain_ref, edge_b1_ref, message_gain_ref, message_bias_ref, w2_ref,
                   edge_ref, mesh_ref, early_ref, late_ref, top_ref, low_ref, *rest):
    going_refs = rest[:-11]
    (x_in, w1_in, vectors_in, edge_in, mesh_in, in_sem, early_sem, weight_sem, edge_sem, going_sem, out_sem) = rest[-11:]
    channels, rows, lanes = x_ref.shape
    latent = w2_ref.shape[0]
    group = CHUNK
    steps = DEPTH // group
    low = (rows - EARLY) // HALO * DEPTH
    end = low + latent
    sources = [w1_ref, b1_ref, gain_ref, edge_b1_ref, message_gain_ref, message_bias_ref]
    targets = [w1_in] + [vectors_in.at[n] for n in range(5)]
    early = [pltpu.make_async_copy(s, t, early_sem.at[n]) for n, (s, t) in enumerate(zip(sources, targets))]
    for copy in early:
        copy.start()
    incoming = []
    for k in range(steps):
        size = min(group, channels - k * group)
        copy = pltpu.make_async_copy(
            x_ref.at[pl.ds(k * group, size)], x_in.at[pl.ds(k * group, size)], in_sem.at[k]
        )
        copy.start()
        incoming.append(copy)
    layers = len(going_refs) + 1
    _, joined = going_refs[0].shape
    share = edge_in.shape[1] // layers
    layer = lax.axis_index("gz")
    features = [
        pltpu.make_async_copy(edge_ref, edge_in, edge_sem.at[0]),
        pltpu.make_async_copy(mesh_ref, mesh_in, edge_sem.at[1]),
    ]
    for copy in features:
        copy.start()
    weight = pltpu.make_async_copy(w2_ref, late_ref.at[pl.ds(low, latent), pl.ds(0, latent)], weight_sem)
    weight.start()
    for copy in early:
        copy.wait()
    stacked = []
    split = [three_parts(vectors_in[n]) for n in range(1, 1 + VECTORS)]
    for n in range(ONES):
        stacked += [parts[n] for parts in split]
    stacked.append(jnp.zeros((lanes - len(stacked), latent), jnp.float32))
    at = latent + 2 * lanes
    late_ref[low:end, at : at + lanes] = jnp.transpose(jnp.concatenate(stacked, axis=0)).astype(jnp.bfloat16)
    bias = three_parts(vectors_in[0]) + [jnp.zeros((DEPTH - channels - ONES, latent), jnp.float32)]
    full = jnp.concatenate([w1_in[...].astype(jnp.float32)] + bias, axis=0) * 0.5
    late_ref[low:end, latent : latent + DEPTH] = jnp.transpose(full).astype(jnp.bfloat16)

    for copy in features:
        copy.wait()
    going = []
    for j, target in enumerate(going_refs):
        first = pl.multiple_of((layer + j + 1) % layers * share, share)
        pair = [
            (edge_in.at[:, pl.ds(first, share)], target.at[:, pl.ds(0, share)]),
            (mesh_in, target.at[:, pl.ds(share, joined - share)]),
        ]
        going += [pltpu.make_async_copy(s, t, going_sem.at[2 * j + n]) for n, (s, t) in enumerate(pair)]
    for copy in going:
        copy.start()

    row_ids = lax.broadcasted_iota(jnp.int32, (group, lanes), 0)
    for k in range(steps):
        incoming[k].wait()
        cells = jnp.swapaxes(x_in[k * group : (k + 1) * group], 0, 1)
        for r in range(rows):
            plane = cells[r]
            if (k + 1) * group > channels:
                ids = row_ids + k * group
                wide = plane.astype(jnp.float32)
                wide = jnp.where(ids < channels, wide, jnp.where(ids < channels + ONES, 1.0, 0.0))
                plane = wide.astype(jnp.bfloat16)
            target, row = (early_ref, r) if r < EARLY else (late_ref, r - EARLY)
            down = row // HALO * DEPTH + k * group
            over = r % HALO * lanes
            target[down : down + group, over : over + lanes] = plane
    ends = [
        pltpu.make_async_copy(early_ref.at[pl.ds(0, DEPTH), :], top_ref, out_sem.at[0]),
        pltpu.make_async_copy(late_ref.at[pl.ds(low - DEPTH, DEPTH), :], low_ref, out_sem.at[1]),
    ]
    for copy in ends:
        copy.start()
    for copy in [weight] + going + ends:
        copy.wait()


def prepare(grid_inputs, w1, b1, gain, edge_b1, message_gain, message_bias, w2, edge_own, mesh_own, layers):
    channels, rows, lanes = grid_inputs.shape
    latent = w1.shape[0]
    steps = DEPTH // CHUNK
    shard, slots = edge_own.shape
    strip = pltpu.VMEM((DEPTH, WIDE), jnp.bfloat16)
    vectors = [a[None] for a in (b1, gain, edge_b1, message_gain, message_bias)]
    return pl.pallas_call(
        prepare_kernel,
        name="prepare",
        compiler_params=pltpu.CompilerParams(vmem_limit_bytes=24 << 20),
        in_specs=[HBM] * 10,
        out_specs=[VMEM] * (layers + 3),
        out_shape=[
            pltpu.VMEM((EARLY // HALO * DEPTH, WIDE), jnp.bfloat16),
            pltpu.VMEM(((rows - EARLY) // HALO * DEPTH + latent, WIDE), jnp.bfloat16),
            strip,
            strip,
        ] + [pltpu.VMEM((shard, slots // layers + mesh_own.shape[1]), jnp.bfloat16)] * (layers - 1),
        scratch_shapes=[
            pltpu.VMEM((DEPTH, rows, lanes), jnp.bfloat16),
            pltpu.VMEM((channels, latent), jnp.bfloat16),
            pltpu.VMEM((5, 1, latent), jnp.float32),
            pltpu.VMEM(edge_own.shape, jnp.bfloat16),
            pltpu.VMEM(mesh_own.shape, jnp.bfloat16),
            pltpu.SemaphoreType.DMA((steps,)),
            pltpu.SemaphoreType.DMA((6,)),
            pltpu.SemaphoreType.DMA,
            pltpu.SemaphoreType.DMA((2,)),
            pltpu.SemaphoreType.DMA((2 * layers - 2,)),
            pltpu.SemaphoreType.DMA((2,)),
        ],
    )(*[off_chip(a) for a in [grid_inputs, w1.T] + vectors + [w2, edge_own, mesh_own]])


def sender_places(senders_ref, slots, rows, lon_bits):
    lanes = LANES
    start = pl.multiple_of(lax.axis_index("gz") * slots, slots)
    cell = senders_ref[:, pl.ds(start, slots)]
    lon_total = 1 << lon_bits
    lat = lax.shift_right_logical(cell, lon_bits) - lax.axis_index("gx") * rows
    lon = ((cell & (lon_total - 1)) - lax.axis_index("gy") * lanes + HALO & (lon_total - 1)) - HALO
    own = rows * lanes
    side = (rows + 2 * HALO) * HALO
    at_row = jnp.where(
        lat < 0, own + (lat + HALO) * lanes, jnp.where(lat < rows, lat * lanes, own + WIDE + (lat - rows) * lanes)
    )
    at_side = own + 2 * WIDE + HALO * jnp.where(lat < 0, rows + lat + HALO, jnp.where(lat < rows, lat, lat + HALO))
    return jnp.where(
        (lon >= 0) & (lon < lanes), at_row + lon, jnp.where(lon < 0, at_side + lon + HALO, at_side + side + lon - lanes)
    )


def picked(parts, begin, places, total):
    slots = places.shape[1]
    for part in parts:
        size = part.shape[1]
        ids = lax.broadcasted_iota(jnp.int32, (size, slots), 0) + begin
        total = total + dot(part, jnp.where(ids == places, 1.0, 0.0).astype(jnp.bfloat16))
        begin += size
    return total


def packed_columns(planes, first_row, left_ref, right_ref):
    lanes = LANES
    per = lanes // HALO
    lane_ids = lax.broadcasted_iota(jnp.int32, (DEPTH, lanes), 1)
    for g, cells in enumerate(planes):
        for k in range(HALO):
            r = first_row + g * HALO + k
            plane = cells[:, k * lanes : (k + 1) * lanes].astype(jnp.float32)
            first = r % per * HALO
            again = (first + HALO) % lanes
            mine = (lane_ids >= first) & (lane_ids < first + HALO)
            moved = pltpu.roll(plane, first, 1) if first else plane
            moved_too = pltpu.roll(plane, again, 1) if again else plane
            left = moved if r % per == 0 else jnp.where(mine, moved, left)
            right = moved_too if r % per == 0 else jnp.where(mine, moved_too, right)
            if r % per == per - 1:
                place = slice(r // per * lanes, (r // per + 1) * lanes)
                left_ref[:, place] = left.astype(jnp.bfloat16)
                right_ref[:, place] = right.astype(jnp.bfloat16)


def own_kernel(count_ref, senders_ref, receivers_ref, early_ref, late_ref,
               left_ref, right_ref, picked_ref, near_ref, live_ref, degree_ref, count, sem, *, rows, lon_bits):
    counting = pltpu.make_async_copy(count_ref, count, sem)
    counting.start()
    slots = picked_ref.shape[1]
    places = sender_places(senders_ref, slots, rows, lon_bits)
    total = jnp.zeros(picked_ref.shape, jnp.float32)
    pair = 2
    for g in range(0, rows // HALO, pair):
        planes = [plane_group(early_ref, late_ref, g + n) for n in range(pair)]
        total = picked(planes, g * WIDE, places, total)
        packed_columns(planes, g * HALO, left_ref, right_ref)
    picked_ref[...] = total

    counting.wait()
    live = count[0, 0]
    nodes = near_ref.shape[0]
    tile = lax.axis_index("gx") * lax.axis_size("gy") + lax.axis_index("gy")
    nt = (((1,), (1,)), ((), ()))
    every = receivers_ref.shape[1]
    slot_all = lax.broadcasted_iota(jnp.int32, (1, every), 1)
    near_all = jnp.where(slot_all < live, receivers_ref[...] - tile * nodes, -1)
    node_all = lax.broadcasted_iota(jnp.int32, (nodes, every), 0)
    counted_all = jnp.where(node_all == near_all, 1.0, 0.0).astype(jnp.bfloat16)
    degree_ref[...] = lax.dot_general(
        jnp.ones((8, every), jnp.bfloat16), counted_all, nt, preferred_element_type=jnp.float32
    )
    start = pl.multiple_of(lax.axis_index("gz") * slots, slots)
    near = receivers_ref[:, pl.ds(start, slots)] - tile * nodes
    node_ids = lax.broadcasted_iota(jnp.int32, (nodes, slots), 0)
    near_ref[...] = jnp.where(node_ids == near, 1.0, 0.0).astype(jnp.bfloat16)
    slot_ids = lax.broadcasted_iota(jnp.int32, (1, slots), 1) + start
    live_ref[...] = jnp.where(node_ids == jnp.where(slot_ids < live, near, -1), 1.0, 0.0).astype(jnp.bfloat16)


def own_work(count, senders, receivers, early, late, rows, slots, nodes, lon_total):
    packed = pltpu.VMEM((DEPTH, (rows + 2 * HALO) * HALO), jnp.bfloat16)
    table = pltpu.VMEM((nodes, slots), jnp.bfloat16)
    return pl.pallas_call(
        functools.partial(own_kernel, rows=rows, lon_bits=lon_total.bit_length() - 1),
        name="own",
        compiler_params=pltpu.CompilerParams(vmem_limit_bytes=32 << 20),
        in_specs=[pl.BlockSpec(memory_space=pl.ANY)] + [VMEM] * 4,
        out_specs=[VMEM] * 6,
        out_shape=[
            packed,
            packed,
            pltpu.VMEM((DEPTH, slots), jnp.float32),
            table,
            table,
            pltpu.VMEM((8, nodes), jnp.float32),
        ],
        scratch_shapes=[pltpu.SMEM((1, 1), jnp.int32), pltpu.SemaphoreType.DMA],
        cost_estimate=pl.CostEstimate(flops=2 * 10**9, transcendentals=0, bytes_accessed=1 << 22),
    )(count, senders, receivers, on_chip(early), on_chip(late))


def strip_kernel(senders_ref, up_ref, down_ref, left_in, right_in, picked_in, left_ref, right_ref, picked_ref, *, rows, lon_bits):
    strips = [up_ref[...], down_ref[...]]
    packed_columns(strips, rows, left_ref, right_ref)
    places = sender_places(senders_ref, picked_ref.shape[1], rows, lon_bits)
    picked_ref[...] = picked(strips, rows * LANES, places, picked_in[...])


def strip_work(senders, up, down, left, right, chosen, rows, lon_total):
    return pl.pallas_call(
        functools.partial(strip_kernel, rows=rows, lon_bits=lon_total.bit_length() - 1),
        name="strips",
        compiler_params=pltpu.CompilerParams(vmem_limit_bytes=16 << 20),
        in_specs=[VMEM] * 6,
        out_specs=[VMEM] * 3,
        out_shape=[pltpu.VMEM(a.shape, a.dtype) for a in (left, right, chosen)],
        input_output_aliases={3: 0, 4: 1, 5: 2},
    )(senders, *[on_chip(a) for a in (up, down, left, right, chosen)])


def embed_kernel(x_ref, late_ref, *rest, first, latent):
    out_ref, wide_ref = rest[-2:]
    keep, rows, lanes = out_ref.shape
    layers = latent // keep
    layer = lax.axis_index("gz")
    low = late_ref.shape[0] - latent
    w1 = late_ref[low:, latent : latent + DEPTH]
    begin = lambda k: pl.multiple_of(low + (layer + k) % layers * keep, keep)
    w2 = jnp.concatenate([late_ref[pl.ds(begin(k), keep), :latent] for k in range(layers)], axis=0)
    gain = column(late_ref, begin(0), keep, latent, 0)
    here = pl.multiple_of((pl.program_id(0) + first) * DEPTH, DEPTH)
    hidden = silu_of_half(dot(w1, x_ref[pl.ds(here, DEPTH), :]))
    values = dot(w2, hidden)
    average, factor = normalized(values)
    done = (values[:keep] - average) * factor * gain
    for r in range(rows):
        wide_ref[pl.ds(r, keep, stride=rows), :] = done[:, r * lanes : (r + 1) * lanes]
    out_ref[...] = wide_ref[...].reshape(keep, rows, lanes).astype(jnp.bfloat16)


def embed_rows(early, late, latent, keep, rows_total, first, count, earlier=None):
    begin = first // HALO
    source, start = (early, begin) if first < EARLY else (late, begin - EARLY // HALO)
    args = [on_chip(source), on_chip(late)]
    in_specs = [VMEM] * 2
    aliases = {}
    if earlier is not None:
        args.append(off_chip(earlier))
        in_specs.append(HBM)
        aliases = {2: 0}
    cells = count * LANES
    return pl.pallas_call(
        functools.partial(embed_kernel, first=start, latent=latent),
        name="embed",
        compiler_params=pltpu.CompilerParams(vmem_limit_bytes=24 << 20),
        grid=(count // HALO,),
        in_specs=in_specs,
        out_specs=pl.BlockSpec((keep, HALO, LANES), lambda i: (0, i + begin, 0)),
        scratch_shapes=[pltpu.VMEM((keep * HALO, LANES), jnp.float32)],
        out_shape=jax.ShapeDtypeStruct((keep, rows_total, LANES), jnp.bfloat16),
        input_output_aliases=aliases,
        cost_estimate=pl.CostEstimate(
            flops=2 * cells * latent * (256 + latent), transcendentals=cells * latent, bytes_accessed=cells * 640
        ),
    )(*args)


def edge_kernel(senders_ref, picked_ref, near_ref, live_ref, late_ref, left_ref, right_ref, *rest,
                lon_bits, rows, layers):
    piece_refs = rest[: layers - 1]
    edge_ref, mesh_ref, w1_ref, w2_ref = rest[layers - 1 : layers + 3]
    own_ref, *sum_refs = rest[layers + 3 : 2 * layers + 3]
    w1_in, w2_in, arrived, sums, sem = rest[2 * layers + 3 :]
    latent, joined = arrived.shape
    shard, nodes = own_ref.shape
    slots = joined - nodes
    layer = lax.axis_index("gz")
    start = pl.multiple_of(layer * slots, slots)
    place = lambda j: pl.ds(pl.multiple_of((layer + j) % layers * shard, shard), shard)
    pairs = [
        (edge_ref.at[:, pl.ds(start, slots)], arrived.at[place(0), pl.ds(0, slots)]),
        (mesh_ref, arrived.at[place(0), pl.ds(slots, nodes)]),
        (w1_ref, w1_in),
        (w2_ref, w2_in),
    ]
    copies = [pltpu.make_async_copy(s, t, sem.at[n]) for n, (s, t) in enumerate(pairs)]
    for copy in copies:
        copy.start()
    for j, piece in enumerate(piece_refs):
        arrived[place(layers - 1 - j), :] = piece[...]

    low = late_ref.shape[0] - latent
    vector = lambda n: column(late_ref, low, latent, latent, n)
    sides = [left_ref[...], right_ref[...]]
    total = picked(sides, (rows + 2 * HALO) * LANES, sender_places(senders_ref, slots, rows, lon_bits), picked_ref[...])
    hidden = silu_of_half(dot(late_ref[low:, latent : latent + DEPTH], total.astype(jnp.bfloat16)))
    values = dot(late_ref[low:, :latent], hidden)
    average, factor = normalized(values)
    send = ((values - average) * factor * vector(0)).astype(jnp.bfloat16)

    nt = (((1,), (1,)), ((), ()))
    for copy in copies:
        copy.wait()
    edge = arrived[:, :slots]
    mesh_cols = dot(arrived[:, slots:], near_ref[...]).astype(jnp.bfloat16)
    stacked = jnp.concatenate([edge, send, mesh_cols], axis=0)
    hidden = silu_of_half(0.5 * (dot(w1_in[...], stacked) + vector(1)))
    second = dot(w2_in[...], hidden)
    average, factor = normalized(second)
    message = edge.astype(jnp.float32) + (second - average) * factor * vector(2) + vector(3)
    sums[...] = lax.dot_general(message.astype(jnp.bfloat16), live_ref[...], nt, preferred_element_type=jnp.float32)
    own_ref[...] = sums[place(0), :]
    for j, target in enumerate(sum_refs):
        target[...] = sums[place(j + 1), :].astype(jnp.bfloat16)


def edge_sums(senders, chosen, near, live, late, left, right, pieces, edge_own, mesh_own, w1, w2,
              rows, lon_total):
    latent = w2.shape[0]
    layers = len(pieces) + 1
    shard, nodes = mesh_own.shape
    slots = edge_own.shape[1] // layers
    near_by = [on_chip(a) for a in (chosen, near, live, late, left, right, *pieces)]
    far = [off_chip(a) for a in (edge_own, mesh_own, w1, w2)]
    return pl.pallas_call(
        functools.partial(edge_kernel, lon_bits=lon_total.bit_length() - 1, rows=rows, layers=layers),
        name="edges",
        compiler_params=pltpu.CompilerParams(vmem_limit_bytes=32 << 20),
        in_specs=[VMEM] * (1 + len(near_by)) + [HBM] * 4,
        out_specs=[VMEM] * layers,
        out_shape=[pltpu.VMEM((shard, nodes), jnp.float32)]
        + [pltpu.VMEM((shard, nodes), jnp.bfloat16)] * (layers - 1),
        scratch_shapes=[
            pltpu.VMEM(w1.shape, jnp.bfloat16),
            pltpu.VMEM(w2.shape, jnp.bfloat16),
            pltpu.VMEM((latent, slots + nodes), jnp.bfloat16),
            pltpu.VMEM((latent, nodes), jnp.float32),
            pltpu.SemaphoreType.DMA((4,)),
        ],
        cost_estimate=pl.CostEstimate(flops=4 * 10**9, transcendentals=0, bytes_accessed=1 << 22),
    )(senders, *near_by, *far)


def finish_kernel(own_ref, *rest):
    *part_refs, degree_ref, mesh_ref, out_ref = rest
    totals = own_ref[...]
    for part in part_refs:
        totals = totals + part[...].astype(jnp.float32)
    scale = jnp.maximum(degree_ref[0:1, :], 1.0)
    out_ref[...] = (mesh_ref[...].astype(jnp.float32) + totals / scale).astype(jnp.bfloat16)


def finish(own, parts, degree, mesh_own):
    args = [on_chip(a) for a in (own, *parts, degree, mesh_own)]
    return pl.pallas_call(
        finish_kernel,
        name="finish",
        compiler_params=pltpu.CompilerParams(vmem_limit_bytes=8 << 20),
        in_specs=[VMEM] * len(args),
        out_specs=VMEM,
        out_shape=jax.ShapeDtypeStruct(mesh_own.shape, jnp.bfloat16),
    )(*args)


def shifted(value, axis, by):
    size = lax.axis_size(axis)
    return lax.ppermute(value, axis, [(i, (i + by) % size) for i in range(size)])


def on_device(
    grid_inputs,
    embed_w1,
    embed_b1,
    embed_w2,
    embed_gain,
    edge_w1,
    edge_b1,
    edge_w2,
    message_gain,
    message_bias,
    mesh_latent,
    edge_latent,
    senders,
    receivers,
    edge_counts,
):
    latent = embed_w2.shape[0]
    shard_rows = mesh_latent.shape[0]
    lat_rows, lon_cols = grid_inputs.shape[1:]
    node_count = mesh_latent.shape[3]
    layers = lax.axis_size("gz")
    lon_total = lon_cols * lax.axis_size("gy")
    mesh_own = mesh_latent[:, 0, 0, :]
    edge_own = edge_latent[:, 0, 0, :]

    early, late, top, low, *outgoing = prepare(
        grid_inputs, embed_w1, embed_b1, embed_gain, edge_b1, message_gain, message_bias, embed_w2, edge_own, mesh_own,
        layers,
    )
    embed = functools.partial(embed_rows, early, late, latent, shard_rows, lat_rows)
    from_up = shifted(low, "gx", 1)
    from_down = shifted(top, "gx", -1)
    pieces = [shifted(piece, "gz", j + 1) for j, piece in enumerate(outgoing)]
    left, right, chosen, near, live, degree = own_work(
        edge_counts, senders[0], receivers[0], early, late, lat_rows, edge_own.shape[1] // layers, mesh_own.shape[1],
        lon_total,
    )
    from_up, from_down, left, right, chosen = lax.optimization_barrier((from_up, from_down, left, right, chosen))
    left, right, chosen = strip_work(senders[0], from_up, from_down, left, right, chosen, lat_rows, lon_total)
    from_left = shifted(right, "gy", 1)
    from_right = shifted(left, "gy", -1)
    grid_out = embed(0, EARLY)
    from_left, from_right, grid_out, *pieces = lax.optimization_barrier((from_left, from_right, grid_out, *pieces))
    own, *sums = edge_sums(
        senders[0], chosen, near, live, late, from_left, from_right, pieces, edge_own, mesh_own, edge_w1, edge_w2,
        lat_rows, lon_total,
    )
    parts = [shifted(part, "gz", j + 1) for j, part in enumerate(sums)]
    grid_out = embed(EARLY, lat_rows - EARLY, grid_out)
    *parts, grid_out = lax.optimization_barrier((*parts, grid_out))
    result = finish(own, parts, degree, mesh_own)
    return (result.reshape(shard_rows, 1, 1, node_count), grid_out)


def solution(mesh):
    return jax.shard_map(
        on_device,
        mesh=mesh,
        in_specs=(
            P(None, "gx", "gy"),
            P(),
            P(),
            P(),
            P(),
            P(),
            P(),
            P(),
            P(),
            P(),
            P("gz", "gx", "gy", None),
            P("gz", "gx", "gy", None),
            P("gx", "gy", None),
            P("gx", "gy", None),
            P("gx", "gy"),
        ),
        out_specs=(P("gz", "gx", "gy", None), P("gz", "gx", "gy")),
        check_vma=False,
    )
```

```python
import functools

import jax
import jax.numpy as jnp
from jax import lax
from jax.experimental import pallas as pl
from jax.experimental.pallas import tpu as pltpu
from jax.sharding import PartitionSpec as P


HALO = 8
LANES = 128
DEPTH = 192
ONES = 3
CHUNK = 16

epsilon = 1e-05


def normalized(values):
    scale = 1.0 / values.shape[0]
    moved = values - values[0:1]
    average = jnp.sum(moved, axis=0, keepdims=True) * scale
    spread = jnp.sum(moved * moved, axis=0, keepdims=True) * scale - average * average
    return moved, average, lax.rsqrt(jnp.maximum(spread, 0.0) + epsilon)


def silu_of_half(half):
    return (half + half * jnp.tanh(half)).astype(jnp.bfloat16)


def dot(a, b):
    return jnp.dot(a, b, preferred_element_type=jnp.float32)


VMEM = pl.BlockSpec(memory_space=pltpu.VMEM)
HBM = pl.BlockSpec(memory_space=pltpu.HBM)


def on_chip(value):
    return pltpu.with_memory_space_constraint(value, pltpu.VMEM)


def off_chip(value):
    return pltpu.with_memory_space_constraint(value, pltpu.HBM)


WIDE = HALO * LANES
VECTORS = 4
PARTS = 2
EARLY = 32


def column(late_ref, begin, count, latent, which):
    at = latent + 2 * LANES
    parts = [
        late_ref[pl.ds(begin, count), at + n * VECTORS + which : at + n * VECTORS + which + 1].astype(jnp.float32)
        for n in range(ONES)
    ]
    return parts[0] + parts[1] + parts[2]


def plane_group(early_ref, late_ref, g):
    k = g - EARLY // HALO
    return early_ref[g * DEPTH : (g + 1) * DEPTH, :] if k < 0 else late_ref[k * DEPTH : (k + 1) * DEPTH, :]


def three_parts(value):
    parts = []
    for _ in range(ONES):
        part = value.astype(jnp.bfloat16).astype(jnp.float32)
        parts.append(part)
        value = value - part
    return parts


def outgoing_kernel(edge_ref, mesh_ref, *rest):
    *going_refs, sem = rest
    layers = len(going_refs) + 1
    _, joined = going_refs[0].shape
    share = edge_ref.shape[1] // layers
    layer = lax.axis_index("gz")
    copies = []
    for j, target in enumerate(going_refs):
        first = pl.multiple_of((layer + j + 1) % layers * share, share)
        pairs = [
            (edge_ref.at[:, pl.ds(first, share)], target.at[:, pl.ds(0, share)]),
            (mesh_ref, target.at[:, pl.ds(share, joined - share)]),
        ]
        copies += [pltpu.make_async_copy(s, t, sem.at[2 * j + n]) for n, (s, t) in enumerate(pairs)]
    for copy in copies:
        copy.start()
    for copy in copies:
        copy.wait()


def outgoing_of(edge_own, mesh_own, layers):
    shard, slots = edge_own.shape
    piece = pltpu.VMEM((shard, slots // layers + mesh_own.shape[1]), jnp.bfloat16)
    return pl.pallas_call(
        outgoing_kernel,
        name="outgoing",
        compiler_params=pltpu.CompilerParams(vmem_limit_bytes=8 << 20),
        in_specs=[HBM] * 2,
        out_specs=[VMEM] * (layers - 1),
        out_shape=[piece] * (layers - 1),
        scratch_shapes=[pltpu.SemaphoreType.DMA((2 * layers - 2,))],
    )(off_chip(edge_own), off_chip(mesh_own))


def prepare_kernel(x_ref, w1_ref, b1_ref, gain_ref, edge_b1_ref, message_gain_ref, message_bias_ref, w2_ref,
                   early_ref, late_ref, top_ref, low_ref, x_in, w1_in, vectors_in, in_sem, early_sem, weight_sem, out_sem):
    channels, rows, lanes = x_ref.shape
    latent = w2_ref.shape[0]
    group = CHUNK
    steps = DEPTH // group
    low = (rows - EARLY) // HALO * DEPTH
    end = low + latent
    sources = [w1_ref, b1_ref, gain_ref, edge_b1_ref, message_gain_ref, message_bias_ref]
    targets = [w1_in] + [vectors_in.at[n] for n in range(5)]
    early = [pltpu.make_async_copy(s, t, early_sem.at[n]) for n, (s, t) in enumerate(zip(sources, targets))]
    for copy in early:
        copy.start()
    incoming = []
    for k in range(steps):
        size = min(group, channels - k * group)
        copy = pltpu.make_async_copy(
            x_ref.at[pl.ds(k * group, size)], x_in.at[pl.ds(k * group, size)], in_sem.at[k]
        )
        copy.start()
        incoming.append(copy)
    weight = pltpu.make_async_copy(w2_ref, late_ref.at[pl.ds(low, latent), pl.ds(0, latent)], weight_sem)
    weight.start()
    for copy in early:
        copy.wait()
    stacked = []
    split = [three_parts(vectors_in[n]) for n in range(1, 1 + VECTORS)]
    for n in range(ONES):
        stacked += [parts[n] for parts in split]
    stacked.append(jnp.zeros((lanes - len(stacked), latent), jnp.float32))
    at = latent + 2 * lanes
    late_ref[low:end, at : at + lanes] = jnp.transpose(jnp.concatenate(stacked, axis=0)).astype(jnp.bfloat16)
    bias = three_parts(vectors_in[0]) + [jnp.zeros((DEPTH - channels - ONES, latent), jnp.float32)]
    full = jnp.concatenate([w1_in[...].astype(jnp.float32)] + bias, axis=0) * 0.5
    late_ref[low:end, latent : latent + DEPTH] = jnp.transpose(full).astype(jnp.bfloat16)

    row_ids = lax.broadcasted_iota(jnp.int32, (group, lanes), 0)
    for k in range(steps):
        incoming[k].wait()
        cells = jnp.swapaxes(x_in[k * group : (k + 1) * group], 0, 1)
        for r in range(rows):
            plane = cells[r]
            if (k + 1) * group > channels:
                ids = row_ids + k * group
                wide = plane.astype(jnp.float32)
                wide = jnp.where(ids < channels, wide, jnp.where(ids < channels + ONES, 1.0, 0.0))
                plane = wide.astype(jnp.bfloat16)
            target, row = (early_ref, r) if r < EARLY else (late_ref, r - EARLY)
            down = row // HALO * DEPTH + k * group
            over = r % HALO * lanes
            target[down : down + group, over : over + lanes] = plane
    ends = [
        pltpu.make_async_copy(early_ref.at[pl.ds(0, DEPTH), :], top_ref, out_sem.at[0]),
        pltpu.make_async_copy(late_ref.at[pl.ds(low - DEPTH, DEPTH), :], low_ref, out_sem.at[1]),
    ]
    for copy in ends:
        copy.start()
    for copy in [weight] + ends:
        copy.wait()


def prepare(grid_inputs, w1, b1, gain, edge_b1, message_gain, message_bias, w2):
    channels, rows, lanes = grid_inputs.shape
    latent = w1.shape[0]
    steps = DEPTH // CHUNK
    strip = pltpu.VMEM((DEPTH, WIDE), jnp.bfloat16)
    vectors = [a[None] for a in (b1, gain, edge_b1, message_gain, message_bias)]
    return pl.pallas_call(
        prepare_kernel,
        name="prepare",
        compiler_params=pltpu.CompilerParams(vmem_limit_bytes=24 << 20),
        in_specs=[HBM] * 8,
        out_specs=[VMEM] * 4,
        out_shape=[
            pltpu.VMEM((EARLY // HALO * DEPTH, WIDE), jnp.bfloat16),
            pltpu.VMEM(((rows - EARLY) // HALO * DEPTH + latent, WIDE), jnp.bfloat16),
            strip,
            strip,
        ],
        scratch_shapes=[
            pltpu.VMEM((DEPTH, rows, lanes), jnp.bfloat16),
            pltpu.VMEM((channels, latent), jnp.bfloat16),
            pltpu.VMEM((5, 1, latent), jnp.float32),
            pltpu.SemaphoreType.DMA((steps,)),
            pltpu.SemaphoreType.DMA((6,)),
            pltpu.SemaphoreType.DMA,
            pltpu.SemaphoreType.DMA((2,)),
        ],
    )(*[off_chip(a) for a in [grid_inputs, w1.T] + vectors + [w2]])


def sender_places(senders_ref, slots, rows, lon_bits):
    lanes = LANES
    start = pl.multiple_of(lax.axis_index("gz") * slots, slots)
    cell = senders_ref[:, pl.ds(start, slots)]
    lon_total = 1 << lon_bits
    lat = lax.shift_right_logical(cell, lon_bits) - lax.axis_index("gx") * rows
    lon = ((cell & (lon_total - 1)) - lax.axis_index("gy") * lanes + HALO & (lon_total - 1)) - HALO
    own = rows * lanes
    side = (rows + 2 * HALO) * HALO
    at_row = jnp.where(
        lat < 0, own + (lat + HALO) * lanes, jnp.where(lat < rows, lat * lanes, own + WIDE + (lat - rows) * lanes)
    )
    at_side = own + 2 * WIDE + HALO * jnp.where(lat < 0, rows + lat + HALO, jnp.where(lat < rows, lat, lat + HALO))
    return jnp.where(
        (lon >= 0) & (lon < lanes), at_row + lon, jnp.where(lon < 0, at_side + lon + HALO, at_side + side + lon - lanes)
    )


def picked(parts, begin, places, total):
    slots = places.shape[1]
    lanes = LANES
    lane_ids = lax.broadcasted_iota(jnp.int32, (lanes, slots), 0)
    in_lane = jnp.where(lane_ids == (places & (lanes - 1)), 1.0, 0.0).astype(jnp.bfloat16)
    plane = lax.shift_right_arithmetic(places, lanes.bit_length() - 1)
    for part in parts:
        size = part.shape[1]
        chosen = [
            in_lane * jnp.where(plane == (begin + at) // lanes, 1.0, 0.0).astype(jnp.bfloat16)
            for at in range(0, size, lanes)
        ]
        total = total + dot(part, jnp.concatenate(chosen, axis=0))
        begin += size
    return total


def packed_columns(planes, first_row, left_ref, right_ref):
    lanes = LANES
    per = lanes // HALO
    lane_ids = lax.broadcasted_iota(jnp.int32, (DEPTH, lanes), 1)
    for g, cells in enumerate(planes):
        for k in range(HALO):
            r = first_row + g * HALO + k
            plane = cells[:, k * lanes : (k + 1) * lanes].astype(jnp.float32)
            first = r % per * HALO
            again = (first + HALO) % lanes
            mine = (lane_ids >= first) & (lane_ids < first + HALO)
            moved = pltpu.roll(plane, first, 1) if first else plane
            moved_too = pltpu.roll(plane, again, 1) if again else plane
            left = moved if r % per == 0 else jnp.where(mine, moved, left)
            right = moved_too if r % per == 0 else jnp.where(mine, moved_too, right)
            if r % per == per - 1:
                place = slice(r // per * lanes, (r // per + 1) * lanes)
                left_ref[:, place] = left.astype(jnp.bfloat16)
                right_ref[:, place] = right.astype(jnp.bfloat16)


def own_kernel(senders_ref, receivers_ref, early_ref, late_ref, left_ref, right_ref, picked_ref, near_ref, *, rows, lon_bits):
    slots = picked_ref.shape[1]
    places = sender_places(senders_ref, slots, rows, lon_bits)
    total = jnp.zeros(picked_ref.shape, jnp.float32)
    pair = 2
    for g in range(0, rows // HALO, pair):
        planes = [plane_group(early_ref, late_ref, g + n) for n in range(pair)]
        total = picked(planes, g * WIDE, places, total)
        packed_columns(planes, g * HALO, left_ref, right_ref)
    picked_ref[...] = total

    nodes = near_ref.shape[0]
    tile = lax.axis_index("gx") * lax.axis_size("gy") + lax.axis_index("gy")
    start = pl.multiple_of(lax.axis_index("gz") * slots, slots)
    near = receivers_ref[:, pl.ds(start, slots)] - tile * nodes
    node_ids = lax.broadcasted_iota(jnp.int32, (nodes, slots), 0)
    near_ref[...] = jnp.where(node_ids == near, 1.0, 0.0).astype(jnp.bfloat16)


def own_work(senders, receivers, early, late, rows, slots, nodes, lon_total):
    packed = pltpu.VMEM((DEPTH, (rows + 2 * HALO) * HALO), jnp.bfloat16)
    table = pltpu.VMEM((nodes, slots), jnp.bfloat16)
    return pl.pallas_call(
        functools.partial(own_kernel, rows=rows, lon_bits=lon_total.bit_length() - 1),
        name="own",
        compiler_params=pltpu.CompilerParams(vmem_limit_bytes=32 << 20),
        in_specs=[VMEM] * 4,
        out_specs=[VMEM] * 4,
        out_shape=[packed, packed, pltpu.VMEM((DEPTH, slots), jnp.float32), table],
        cost_estimate=pl.CostEstimate(flops=2 * 10**9, transcendentals=0, bytes_accessed=1 << 22),
    )(senders, receivers, on_chip(early), on_chip(late))


def strip_kernel(senders_ref, up_ref, down_ref, left_in, right_in, picked_in, left_ref, right_ref, picked_ref, *, rows, lon_bits):
    strips = [up_ref[...], down_ref[...]]
    packed_columns(strips, rows, left_ref, right_ref)
    places = sender_places(senders_ref, picked_ref.shape[1], rows, lon_bits)
    picked_ref[...] = picked(strips, rows * LANES, places, picked_in[...])


def strip_work(senders, up, down, left, right, chosen, rows, lon_total):
    return pl.pallas_call(
        functools.partial(strip_kernel, rows=rows, lon_bits=lon_total.bit_length() - 1),
        name="strips",
        compiler_params=pltpu.CompilerParams(vmem_limit_bytes=16 << 20),
        in_specs=[VMEM] * 6,
        out_specs=[VMEM] * 3,
        out_shape=[pltpu.VMEM(a.shape, a.dtype) for a in (left, right, chosen)],
        input_output_aliases={3: 0, 4: 1, 5: 2},
    )(senders, *[on_chip(a) for a in (up, down, left, right, chosen)])


def embed_kernel(x_ref, late_ref, *rest, start, first, blocks, latent):
    out_ref, wide_ref, done_ref, sem = rest[-4:]
    keep = out_ref.shape[0]
    lanes = LANES
    layers = latent // keep
    layer = lax.axis_index("gz")
    low = late_ref.shape[0] - latent
    w1 = late_ref[low:, latent : latent + DEPTH]
    begin = lambda k: pl.multiple_of(low + (layer + k) % layers * keep, keep)
    w2 = jnp.concatenate([late_ref[pl.ds(begin(k), keep), :latent] for k in range(layers)], axis=0)
    gain = column(late_ref, begin(0), keep, latent, 0)

    def hidden_of(i):
        at = (start + i) * DEPTH
        return silu_of_half(dot(w1, x_ref[at : at + DEPTH, :]))

    copies = []
    hidden = hidden_of(0)
    for i in range(blocks):
        values = dot(w2, hidden)
        following = hidden_of(i + 1) if i + 1 < blocks else None
        moved, average, factor = normalized(values)
        done = (moved[:keep] - average) * factor * gain
        for r in range(HALO):
            wide_ref[i % 2, pl.ds(r, keep, stride=HALO), :] = done[:, r * lanes : (r + 1) * lanes]
        done_ref[i] = wide_ref[i % 2].reshape(keep, HALO, lanes).astype(jnp.bfloat16)
        copy = pltpu.make_async_copy(done_ref.at[i], out_ref.at[:, pl.ds((first + i) * HALO, HALO), :], sem.at[i])
        copy.start()
        copies.append(copy)
        hidden = following
    for copy in copies:
        copy.wait()


def embed_rows(early, late, latent, keep, rows_total, first, count, earlier=None):
    begin = first // HALO
    blocks = count // HALO
    source, start = (early, begin) if first < EARLY else (late, begin - EARLY // HALO)
    args = [on_chip(source), on_chip(late)]
    in_specs = [VMEM] * 2
    aliases = {}
    if earlier is not None:
        args.append(off_chip(earlier))
        in_specs.append(HBM)
        aliases = {2: 0}
    cells = count * LANES
    return pl.pallas_call(
        functools.partial(embed_kernel, start=start, first=begin, blocks=blocks, latent=latent),
        name="embed",
        compiler_params=pltpu.CompilerParams(vmem_limit_bytes=32 << 20),
        in_specs=in_specs,
        out_specs=HBM,
        scratch_shapes=[
            pltpu.VMEM((2, keep * HALO, LANES), jnp.float32),
            pltpu.VMEM((blocks, keep, HALO, LANES), jnp.bfloat16),
            pltpu.SemaphoreType.DMA((blocks,)),
        ],
        out_shape=pltpu.HBM((keep, rows_total, LANES), jnp.bfloat16),
        input_output_aliases=aliases,
        cost_estimate=pl.CostEstimate(
            flops=2 * cells * latent * (256 + latent), transcendentals=cells * latent, bytes_accessed=cells * 640
        ),
    )(*args)


def counts_of(near, nodes):
    every = near.shape[1]
    base = 16
    bits = base.bit_length() - 1
    tops = nodes // base
    digit = lambda count, value: jnp.where(
        lax.broadcasted_iota(jnp.int32, (count, every), 0) == value, 1.0, 0.0
    ).astype(jnp.bfloat16)
    pairs = lax.dot_general(
        digit(tops, lax.shift_right_arithmetic(near, bits)),
        digit(base, near & (base - 1)),
        (((1,), (1,)), ((), ())),
        preferred_element_type=jnp.float32,
    )
    large = jnp.floor(pairs * (1.0 / 128.0))
    small = pairs - 128.0 * large
    columns = lax.broadcasted_iota(jnp.int32, (base, nodes), 1)
    spread = jnp.where((columns & (base - 1)) == lax.broadcasted_iota(jnp.int32, (base, nodes), 0), 1.0, 0.0)
    spread = spread.astype(jnp.bfloat16)
    rows = 128.0 * dot(large.astype(jnp.bfloat16), spread) + dot(small.astype(jnp.bfloat16), spread)
    node_ids = lax.broadcasted_iota(jnp.int32, (tops, nodes), 1)
    mine = lax.shift_right_arithmetic(node_ids, bits) == lax.broadcasted_iota(jnp.int32, (tops, nodes), 0)
    return jnp.sum(jnp.where(mine, rows, 0.0), axis=0, keepdims=True)


def first_kernel(count_ref, receivers_ref, near_ref, late_ref, *rest, layers):
    piece_refs = rest[: layers - 1]
    edge_ref, mesh_ref, w1_ref, base_ref, all_edge_ref, live_ref, degree_ref, w1_in, arrived, sem = rest[layers - 1 :]
    latent, joined = arrived.shape
    shard = latent // layers
    slots = near_ref.shape[1]
    layer = lax.axis_index("gz")
    start = pl.multiple_of(layer * slots, slots)
    place = lambda j: pl.ds(pl.multiple_of((layer + j) % layers * shard, shard), shard)
    pairs = [
        (edge_ref.at[:, pl.ds(start, slots)], arrived.at[place(0), pl.ds(0, slots)]),
        (mesh_ref, arrived.at[place(0), pl.ds(slots, joined - slots)]),
        (w1_ref.at[:, pl.ds(0, latent)], w1_in.at[0]),
        (w1_ref.at[:, pl.ds(2 * latent, latent)], w1_in.at[1]),
    ]
    copies = [pltpu.make_async_copy(s, t, sem.at[n]) for n, (s, t) in enumerate(pairs)]
    for copy in copies:
        copy.start()
    for j, piece in enumerate(piece_refs):
        arrived[place(layers - 1 - j), :] = piece[...]
    live = count_ref[0, 0]
    nodes = near_ref.shape[0]
    tile = lax.axis_index("gx") * lax.axis_size("gy") + lax.axis_index("gy")
    every = receivers_ref.shape[1]
    slot_all = lax.broadcasted_iota(jnp.int32, (1, every), 1)
    near_all = jnp.where(slot_all < live, receivers_ref[...] - tile * nodes, -1)
    degree_ref[...] = jnp.broadcast_to(counts_of(near_all, nodes), degree_ref.shape)
    slot_ids = lax.broadcasted_iota(jnp.int32, (1, slots), 1) + start
    live_ref[...] = jnp.where(slot_ids < live, near_ref[...].astype(jnp.float32), 0.0).astype(jnp.bfloat16)
    low = late_ref.shape[0] - latent
    for copy in copies:
        copy.wait()
    edge = arrived[:, :slots]
    mesh_cols = dot(arrived[:, slots:], near_ref[...]).astype(jnp.bfloat16)
    both = dot(w1_in[0], edge) + dot(w1_in[1], mesh_cols)
    base_ref[...] = 0.5 * (both + column(late_ref, low, latent, latent, 1))
    all_edge_ref[...] = edge


def first_layer(count, receivers, near, late, pieces, edge_own, mesh_own, w1, layers):
    latent = w1.shape[0]
    slots = near.shape[1]
    near_by = [on_chip(a) for a in (near, late, *pieces)]
    far = [off_chip(a) for a in (edge_own, mesh_own, w1)]
    return pl.pallas_call(
        functools.partial(first_kernel, layers=layers),
        name="first",
        compiler_params=pltpu.CompilerParams(vmem_limit_bytes=24 << 20),
        in_specs=[pl.BlockSpec(memory_space=pltpu.SMEM), VMEM] + [VMEM] * len(near_by) + [HBM] * 3,
        out_specs=[VMEM] * 4,
        out_shape=[
            pltpu.VMEM((latent, slots), jnp.float32),
            pltpu.VMEM((latent, slots), jnp.bfloat16),
            pltpu.VMEM(near.shape, jnp.bfloat16),
            pltpu.VMEM((8, near.shape[0]), jnp.float32),
        ],
        scratch_shapes=[
            pltpu.VMEM((2, latent, latent), jnp.bfloat16),
            pltpu.VMEM((latent, slots + mesh_own.shape[1]), jnp.bfloat16),
            pltpu.SemaphoreType.DMA((4,)),
        ],
        cost_estimate=pl.CostEstimate(flops=10**9, transcendentals=0, bytes_accessed=1 << 22),
    )(count, receivers, *near_by, *far)


def edge_kernel(senders_ref, picked_ref, live_ref, late_ref, left_ref, right_ref, base_ref, all_edge_ref, w1_ref, w2_ref,
                own_ref, *rest, lon_bits, rows, layers):
    sum_refs = rest[: layers - 1]
    w1_in, w2_in, sums, sem = rest[layers - 1 :]
    latent, slots = base_ref.shape
    shard = latent // layers
    layer = lax.axis_index("gz")
    place = lambda j: pl.ds(pl.multiple_of((layer + j) % layers * shard, shard), shard)
    copies = [
        pltpu.make_async_copy(w1_ref.at[:, pl.ds(latent, latent)], w1_in, sem.at[0]),
        pltpu.make_async_copy(w2_ref, w2_in, sem.at[1]),
    ]
    for copy in copies:
        copy.start()
    low = late_ref.shape[0] - latent
    vector = lambda n: column(late_ref, low, latent, latent, n)
    sides = [left_ref[...], right_ref[...]]
    spots = sender_places(senders_ref, slots, rows, lon_bits)
    nt = (((1,), (1,)), ((), ()))
    part = slots // PARTS
    spans = [slice(h * part, (h + 1) * part) for h in range(PARTS)]
    total = [picked(sides, (rows + 2 * HALO) * LANES, spots[:, h], picked_ref[:, h]).astype(jnp.bfloat16) for h in spans]
    w1, w2 = late_ref[low:, latent : latent + DEPTH], late_ref[low:, :latent]
    hidden = [silu_of_half(dot(w1, t)) for t in total]
    values = [dot(w2, t) for t in hidden]
    send = []
    for v in values:
        moved, average, factor = normalized(v)
        send.append(((moved - average) * factor * vector(0)).astype(jnp.bfloat16))
    for copy in copies:
        copy.wait()
    hidden = [silu_of_half(base_ref[:, h] + 0.5 * dot(w1_in[...], t)) for h, t in zip(spans, send)]
    second = [dot(w2_in[...], t) for t in hidden]
    added = None
    for h, v in zip(spans, second):
        moved, average, factor = normalized(v)
        message = all_edge_ref[:, h].astype(jnp.float32) + (moved - average) * factor * vector(2) + vector(3)
        partial = lax.dot_general(
            message.astype(jnp.bfloat16), live_ref[:, h], nt, preferred_element_type=jnp.float32
        )
        added = partial if added is None else added + partial
    sums[...] = added
    own_ref[...] = sums[place(0), :]
    for j, target in enumerate(sum_refs):
        target[...] = sums[place(j + 1), :].astype(jnp.bfloat16)


def edge_sums(senders, chosen, live, late, left, right, base, all_edge, w1, w2, layers, rows, lon_total):
    latent = w2.shape[0]
    nodes = live.shape[0]
    shard = latent // layers
    near_by = [on_chip(a) for a in (chosen, live, late, left, right, base, all_edge)]
    return pl.pallas_call(
        functools.partial(edge_kernel, lon_bits=lon_total.bit_length() - 1, rows=rows, layers=layers),
        name="edges",
        compiler_params=pltpu.CompilerParams(vmem_limit_bytes=32 << 20),
        in_specs=[VMEM] * (1 + len(near_by)) + [HBM] * 2,
        out_specs=[VMEM] * layers,
        out_shape=[pltpu.VMEM((shard, nodes), jnp.float32)]
        + [pltpu.VMEM((shard, nodes), jnp.bfloat16)] * (layers - 1),
        scratch_shapes=[
            pltpu.VMEM((latent, latent), jnp.bfloat16),
            pltpu.VMEM(w2.shape, jnp.bfloat16),
            pltpu.VMEM((latent, nodes), jnp.float32),
            pltpu.SemaphoreType.DMA((2,)),
        ],
        cost_estimate=pl.CostEstimate(flops=3 * 10**9, transcendentals=0, bytes_accessed=1 << 22),
    )(senders, *near_by, off_chip(w1), off_chip(w2))


def finish_kernel(own_ref, *rest):
    *part_refs, degree_ref, mesh_ref, out_ref = rest
    totals = own_ref[...]
    for part in part_refs:
        totals = totals + part[...].astype(jnp.float32)
    scale = jnp.maximum(degree_ref[0:1, :], 1.0)
    out_ref[...] = (mesh_ref[...].astype(jnp.float32) + totals / scale).astype(jnp.bfloat16)


def finish(own, parts, degree, mesh_own):
    args = [on_chip(a) for a in (own, *parts, degree, mesh_own)]
    return pl.pallas_call(
        finish_kernel,
        name="finish",
        compiler_params=pltpu.CompilerParams(vmem_limit_bytes=8 << 20),
        in_specs=[VMEM] * len(args),
        out_specs=VMEM,
        out_shape=jax.ShapeDtypeStruct(mesh_own.shape, jnp.bfloat16),
    )(*args)


def shifted(value, axis, by):
    size = lax.axis_size(axis)
    return lax.ppermute(value, axis, [(i, (i + by) % size) for i in range(size)])


def on_device(
    grid_inputs,
    embed_w1,
    embed_b1,
    embed_w2,
    embed_gain,
    edge_w1,
    edge_b1,
    edge_w2,
    message_gain,
    message_bias,
    mesh_latent,
    edge_latent,
    senders,
    receivers,
    edge_counts,
):
    latent = embed_w2.shape[0]
    shard_rows = mesh_latent.shape[0]
    lat_rows, lon_cols = grid_inputs.shape[1:]
    node_count = mesh_latent.shape[3]
    layers = lax.axis_size("gz")
    lon_total = lon_cols * lax.axis_size("gy")
    mesh_own = mesh_latent[:, 0, 0, :]
    edge_own = edge_latent[:, 0, 0, :]

    outgoing = outgoing_of(edge_own, mesh_own, layers)
    early, late, top, low = prepare(
        grid_inputs, embed_w1, embed_b1, embed_gain, edge_b1, message_gain, message_bias, embed_w2
    )
    embed = functools.partial(embed_rows, early, late, latent, shard_rows, lat_rows)
    from_up = shifted(low, "gx", 1)
    from_down = shifted(top, "gx", -1)
    pieces = [shifted(piece, "gz", j + 1) for j, piece in enumerate(outgoing)]
    left, right, chosen, near = own_work(
        senders[0], receivers[0], early, late, lat_rows, edge_own.shape[1] // layers, mesh_own.shape[1],
        lon_total,
    )
    from_up, from_down, left, right, chosen = lax.optimization_barrier((from_up, from_down, left, right, chosen))
    left, right, chosen = strip_work(senders[0], from_up, from_down, left, right, chosen, lat_rows, lon_total)
    from_left = shifted(right, "gy", 1)
    from_right = shifted(left, "gy", -1)
    grid_out = embed(0, EARLY)
    *pieces, grid_out, edge_counts = lax.optimization_barrier((*pieces, grid_out, edge_counts))
    base, all_edge, live, degree = first_layer(edge_counts, receivers[0], near, late, pieces, edge_own, mesh_own, edge_w1, layers)
    from_left, from_right, base, grid_out = lax.optimization_barrier((from_left, from_right, base, grid_out))
    own, *sums = edge_sums(
        senders[0], chosen, live, late, from_left, from_right, base, all_edge, edge_w1, edge_w2, layers, lat_rows, lon_total
    )
    parts = [shifted(part, "gz", j + 1) for j, part in enumerate(sums)]
    grid_out = embed(EARLY, lat_rows - EARLY, grid_out)
    *parts, grid_out = lax.optimization_barrier((*parts, grid_out))
    result = finish(own, parts, degree, mesh_own)
    return (result.reshape(shard_rows, 1, 1, node_count), grid_out)


def solution(mesh):
    return jax.shard_map(
        on_device,
        mesh=mesh,
        in_specs=(
            P(None, "gx", "gy"),
            P(),
            P(),
            P(),
            P(),
            P(),
            P(),
            P(),
            P(),
            P(),
            P("gz", "gx", "gy", None),
            P("gz", "gx", "gy", None),
            P("gx", "gy", None),
            P("gx", "gy", None),
            P("gx", "gy"),
        ),
        out_specs=(P("gz", "gx", "gy", None), P("gz", "gx", "gy")),
        check_vma=False,
    )
```
